256 devices in a mesh: shard: 16 (over z, core), tp: 4 (over y), shift: 4 (over x).
Axes of the slice: x: 4, y: 4, z: 8, core: 2. Of those that a mesh axis runs over, the one named last changes fastest.
Arguments:
- weight_query: bfloat16 [10240, 4096], P(('shift', 'shard'), 'tp'), parts along dimension 0, may hold values from -0.15625 to 0.15625
- low_query: bfloat16 [10240, 64], P(('shift', 'shard')), parts along dimension 0, may hold values from -0.125 to 0.125
- high_query: bfloat16 [256, 4096], P('shift', 'tp'), parts along dimension 0, may hold values from -0.75 to 0.75
- weight_key: bfloat16 [10240, 1024], P(('shift', 'shard'), 'tp'), parts along dimension 0, may hold values from -0.15625 to 0.15625
- low_key: bfloat16 [10240, 64], P(('shift', 'shard')), parts along dimension 0, may hold values from -0.125 to 0.125
- high_key: bfloat16 [256, 1024], P('shift', 'tp'), parts along dimension 0, may hold values from -0.75 to 0.75
- weight_value: bfloat16 [10240, 1024], P(('shift', 'shard'), 'tp'), parts along dimension 0, may hold values from -0.15625 to 0.15625
- low_value: bfloat16 [10240, 64], P(('shift', 'shard')), parts along dimension 0, may hold values from -0.125 to 0.125
- high_value: bfloat16 [256, 1024], P('shift', 'tp'), parts along dimension 0, may hold values from -0.75 to 0.75
- norm_train: float32 [10240], P(('shift', 'shard', 'tp')), parts along dimension 0, may hold values from 0.25 to 1.75
- norm_step: float32 [10240], P(('shift', 'shard', 'tp')), parts along dimension 0, may hold values from -0.3 to 0.3
Outputs:
- serve_query: bfloat16 [10240, 4096], P('shift', 'tp'), parts along dimension 0
- serve_key: bfloat16 [10240, 1024], P('shift', 'tp'), parts along dimension 0
- serve_value: bfloat16 [10240, 1024], P('shift', 'tp'), parts along dimension 0
- factor_query: float32 [16384], P(('shift', 'tp')), parts along dimension 0
- factor_key: float32 [4096], P(('shift', 'tp')), parts along dimension 0
- factor_value: float32 [4096], P(('shift', 'tp')), parts along dimension 0
- serve_norm: bfloat16 [10240], P('shift'), parts along dimension 0
The draws below stay inside these ranges and needn't reach their ends.
There are 4 independent parts, one for each index of `shift`. The reference program is written for one: setup_inputs(seed, part) draws one part's arguments, and reference() takes and returns one part's arrays. A program takes and returns all parts, laid end to end along the dimension named above; each array names one. Nothing has to cross between parts.
All inputs are finite; a program needn't handle non-finite values. Where the reference program divides by a largest or mean magnitude, that divisor is 1e-20 or more.
Results may differ from the reference program's by a relative error of at most 0.001.
Values may be sent and summed in bfloat16 or wider, within the bound.
A program may use at most 64 MiB of HBM per device.

```python
import jax
import jax.numpy as jnp

D_MODEL = 2560
Q_DIM = 4096
KV_DIM = 1024
RANK = 64


def with_spikes(entries, stream_key, source, target, shards_of, factor):
    owner, partner = [(jnp.arange(entries.shape[dim]) // (entries.shape[dim] // shards_of)).reshape([-1 if axis == dim else 1 for axis in range(entries.ndim)]) for dim in (source, target)]
    chosen = jax.random.permutation(stream_key, shards_of)[partner]
    strong = (owner == chosen) | (owner == (partner + shards_of // 2) % shards_of)
    return jnp.where(strong, factor * entries, entries)


def level_of(key, extent, cuts, least, largest):
    def one(position, parts):
        steps = jax.random.uniform(jax.random.fold_in(jax.random.fold_in(key, 6), position), (parts,), jnp.float32, least / len(cuts), largest / len(cuts))
        return jnp.repeat(jnp.exp(steps), extent[position] // parts).reshape((-1,) + (1,) * (len(extent) - position - 1))

    level = one(*cuts[0])
    for cut in cuts[1:]:
        level = level * one(*cut)
    return level


def bell_draw(stream_key, shape, deviation, reach, split=(), kind=jnp.bfloat16):
    values = jax.random.normal(stream_key, shape, jnp.float32) * deviation
    if len(split) > 0:
        values = level_of(stream_key, shape, split, -0.22, 0.18) * values
    return jnp.clip(values, min=-reach, max=reach).astype(kind)


def bell_draw_with(stream_key, dims, deviation, most, cuts, heavy, held_as=jnp.bfloat16):
    entries = deviation * jax.random.normal(stream_key, dims, jnp.float32)
    if cuts:
        entries = entries * level_of(stream_key, dims, cuts, -0.22, 0.18)
    return jnp.clip(with_spikes(entries, jax.random.fold_in(stream_key, 3), *heavy), -most, most).astype(held_as)


def setup_inputs(seed: int = 0, part: int = 0) -> dict:
    arg_keys = jax.random.split(jax.random.key(seed), 12)
    part_splits = jax.random.split(jax.random.fold_in(arg_keys[11], part), 12)
    weight_query = bell_draw_with(part_splits[0], (D_MODEL, Q_DIM), D_MODEL ** -0.5, 0.15625, ((0, 16), (1, 4)), (0, 1, 16, 2.0))
    low_query = bell_draw(part_splits[1], (D_MODEL, RANK), D_MODEL ** -0.5, 0.125, ((0, 16),))
    high_query = bell_draw(part_splits[2], (RANK, Q_DIM), RANK ** -0.5, 0.75, ((1, 4),))
    weight_key = bell_draw_with(part_splits[3], (D_MODEL, KV_DIM), D_MODEL ** -0.5, 0.15625, ((0, 16), (1, 4)), (0, 1, 16, 2.0))
    low_key = bell_draw(part_splits[4], (D_MODEL, RANK), D_MODEL ** -0.5, 0.125, ((0, 16),))
    high_key = bell_draw(part_splits[5], (RANK, KV_DIM), RANK ** -0.5, 0.75, ((1, 4),))
    weight_value = bell_draw_with(part_splits[6], (D_MODEL, KV_DIM), D_MODEL ** -0.5, 0.15625, ((0, 16), (1, 4)), (0, 1, 16, 2.0))
    low_value = bell_draw(part_splits[7], (D_MODEL, RANK), D_MODEL ** -0.5, 0.125, ((0, 16),))
    high_value = bell_draw(part_splits[8], (RANK, KV_DIM), RANK ** -0.5, 0.75, ((1, 4),))
    norm_train = jnp.clip(1.0 + 0.15 * jax.random.normal(part_splits[9], (D_MODEL,), jnp.float32), 0.25, 1.75)
    norm_step = jnp.clip(jax.random.uniform(part_splits[10], (D_MODEL,), jnp.float32, -0.3, 0.3) * level_of(part_splits[10], (D_MODEL,), ((0, 64),), -0.4, 0.0), -0.3, 0.3)
    return dict(weight_query=weight_query, low_query=low_query, high_query=high_query, weight_key=weight_key, low_key=low_key, high_key=high_key, weight_value=weight_value, low_value=low_value, high_value=high_value, norm_train=norm_train, norm_step=norm_step)


mix_rate = 1.0


def reference(weight_query, low_query, high_query, weight_key, low_key, high_key, weight_value, low_value, high_value, norm_train, norm_step):
    fresh_query = weight_query.astype(jnp.float32) + mix_rate * jnp.dot(low_query, high_query, preferred_element_type=jnp.float32)
    fresh_key = weight_key.astype(jnp.float32) + mix_rate * jnp.dot(low_key, high_key, preferred_element_type=jnp.float32)
    fresh_value = weight_value.astype(jnp.float32) + mix_rate * jnp.dot(low_value, high_value, preferred_element_type=jnp.float32)
    factor_query = jnp.sum(jnp.abs(fresh_query), axis=0) / D_MODEL
    serve_query = (fresh_query / factor_query).astype(jnp.bfloat16)
    factor_key = jnp.sum(jnp.abs(fresh_key), axis=0) / D_MODEL
    serve_key = (fresh_key / factor_key).astype(jnp.bfloat16)
    factor_value = jnp.sum(jnp.abs(fresh_value), axis=0) / D_MODEL
    serve_value = (fresh_value / factor_value).astype(jnp.bfloat16)
    serve_norm = (norm_train + norm_step).astype(jnp.bfloat16)
    return serve_query, serve_key, serve_value, factor_query, factor_key, factor_value, serve_norm
```

```python
import functools

import jax
import jax.numpy as jnp
from jax import lax
from jax.experimental import pallas as pl
from jax.experimental.pallas import tpu as pltpu
from jax.sharding import PartitionSpec as P

MESH = pl.DeviceIdType.MESH
F32 = jnp.float32
BF16 = jnp.bfloat16

mix_rate = 1.0

CHUNKS = ((1, 0, 160), (2, 0, 160), (0, 0, 48), (0, 48, 64), (0, 112, 48))
LAST = ((0, 1, 2), (3, 4))
COLS = (0, 1024, 1280, 1536)
TILE = 256


def kernel(
    wq, lq, hq, wk, lk, hk, wv, lv, hv, nt, ns,
    oq, ok, ov, fq, fk, fv, on,
    sw0, sw1, sw2, sl0, sl1, sl2, sh0, sh1, sh2, snt, sns,
    rw0, rw1, rw2, rl0, rl1, rl2, prod,
    st, stp, msg, gath, fin, nrm, nall, inv, nout, nrow,
    load_sem, sr_send, sr_recv, st_send, st_recv, g_send, g_recv, f_send, f_recv,
    n_send, n_recv, y_send, y_recv, low_send, low_recv, r_send, r_recv, p_send, p_recv,
):
    shard = lax.axis_index("shard")
    y = lax.axis_index("tp")
    z, c = shard // 2, shard % 2
    nz = 8
    rows = wq.shape[0]
    d_model = rows * 16
    outs = (oq, ok, ov)
    w = (sw0, sw1, sw2)
    low = (sl0, sl1, sl2)
    high = (sh0, sh1, sh2)
    rw = (rw0, rw1, rw2)
    rl = (rl0, rl1, rl2)
    step = (1 - 2 * c, 2 * c - 1)

    def at(zz, cc):
        return {"shard": lax.rem(zz + 4 * nz, nz) * 2 + cc}

    partner = at(z, 1 - c)
    nbr = (at(z + step[0], c), at(z + step[1], c))

    loads = []
    for i, (src, dst) in enumerate(
        zip((wk, wv, wq, lq, lk, lv, hq, hk, hv, nt, ns), (sw1, sw2, sw0, sl0, sl1, sl2, sh0, sh1, sh2, snt, sns))
    ):
        cp = pltpu.make_async_copy(src, dst, load_sem.at[i])
        cp.start()
        loads.append(cp)

    barrier = pltpu.get_barrier_semaphore()
    peers = [at(z + d, c) for d in range(1, nz)] + [partner] + [{"tp": lax.rem(y + d, 4)} for d in range(1, 4)]
    for peer in peers:
        pl.semaphore_signal(barrier, inc=1, device_id=peer, device_id_type=MESH)
    for cp in loads:
        cp.wait()
    pl.semaphore_wait(barrier, len(peers))

    sends = []

    def send(src, dst, s_sem, r_sem, to):
        cp = pltpu.make_async_remote_copy(
            src_ref=src, dst_ref=dst, send_sem=s_sem, recv_sem=r_sem, device_id=to, device_id_type=MESH
        )
        cp.start()
        sends.append(cp)

    def arrived(dst, sem):
        pltpu.make_async_remote_copy(
            src_ref=dst, dst_ref=dst, send_sem=sem, recv_sem=sem, device_id=partner, device_id_type=MESH
        ).wait_recv()

    def send_raw(i):
        a, r0, n = CHUNKS[i]
        for d in range(2):
            send(w[a].at[pl.ds(r0, n)], rw[a].at[d, pl.ds(r0, n)], r_send.at[d, 0, i], r_recv.at[d, 0, i], nbr[d])

    send_raw(0)

    def product(l_ref, h_ref, out, a):
        for t in range(0, COLS[a + 1] - COLS[a], TILE):
            out[:, COLS[a] + t : COLS[a] + t + TILE] = mix_rate * lax.dot_general(
                l_ref[...], h_ref[:, t : t + TILE], (((0,), (0,)), ((), ())), preferred_element_type=F32
            )

    for a in range(3):
        product(low[a], high[a], prod.at[2], a)
    st[...] = jnp.zeros_like(st)
    for a in range(3):
        for t in range(0, COLS[a + 1] - COLS[a], TILE):
            col = COLS[a] + t
            fresh = w[a][:, t : t + TILE].astype(F32) + prod[2, :, col : col + TILE]
            prod[2, :, col : col + TILE] = fresh
            total = jnp.sum(jnp.abs(fresh), axis=0, keepdims=True)
            for g in range(TILE // 128):
                j = col // 128 + g
                st[j // 6, j % 6 : j % 6 + 1, :] = total[:, 128 * g : 128 * (g + 1)]

    send(st.at[1 - c], stp, sr_send, sr_recv, partner)
    arrived(stp, sr_recv)
    msg[0:6, :] = st[c, 0:6, :] + stp[0:6, :]
    msg[6:8, :] = jnp.zeros((2, 128), F32)
    msg[6:7, 0:40] = (snt[...] + sns[...]).reshape(1, 40)
    gath[z] = msg[...]
    for d in range(1, nz):
        send(msg, gath.at[z], g_send.at[d - 1], g_recv.at[d - 1], at(z + d, c))
    for d in range(2):
        for a in range(3):
            send(low[a], rl[a].at[d], low_send.at[d, a], low_recv.at[d, a], nbr[d])
    for i in range(1, len(CHUNKS)):
        send_raw(i)

    for d in range(1, nz):
        arrived(gath.at[lax.rem(z - d + nz, nz)], g_recv.at[d - 1])
    total = gath[0]
    for k in range(1, nz):
        total = total + gath[k]
    fin[c] = total * (1.0 / d_model)
    for k in range(nz):
        nrm[c, k : k + 1, :] = gath[k, 6:7, :]
    send(fin.at[c], fin.at[c], f_send, f_recv, partner)
    send(nrm.at[c], nrm.at[c], n_send, n_recv, partner)
    arrived(fin.at[1 - c], f_recv)
    for j in range(12):
        row = fin[j // 6, j % 6 : j % 6 + 1, :]
        inv[:, 128 * j : 128 * (j + 1)] = 1.0 / row
        if j < 8:
            fq[:, 128 * j : 128 * (j + 1)] = row
        elif j < 10:
            fk[:, 128 * (j - 8) : 128 * (j - 7)] = row
        else:
            fv[:, 128 * (j - 10) : 128 * (j - 9)] = row

    def place(a, zz, cc, r0, n):
        first = pl.multiple_of((lax.rem(zz + 4 * nz, nz) * 2 + cc) * rows, 16)
        return outs[a].at[pl.ds(first + r0, n)]

    def origin(d, h):
        return z - h * step[d]

    for i, (a, r0, n) in enumerate(CHUNKS):
        dst = place(a, z, c, r0, n)
        for t in range(0, COLS[a + 1] - COLS[a], TILE):
            col = COLS[a] + t
            dst[:, t : t + TILE] = (prod[2, r0 : r0 + n, col : col + TILE] * inv[:, col : col + TILE]).astype(BF16)
        send(dst, dst, p_send.at[0, 0, i], p_recv.at[0, 0, i], partner)

    for d in range(2):
        for a in range(3):
            arrived(rl[a].at[d], low_recv.at[d, a])
            product(rl[a].at[d], high[a], prod.at[d], a)
    for i, (a, r0, n) in enumerate(CHUNKS):
        for d in range(2):
            arrived(rw[a].at[d, pl.ds(r0, n)], r_recv.at[d, 0, i])
            dst = place(a, origin(d, 1), c, r0, n)
            for t in range(0, COLS[a + 1] - COLS[a], TILE):
                col = COLS[a] + t
                fresh = rw[a][d, r0 : r0 + n, t : t + TILE].astype(F32) + prod[d, r0 : r0 + n, col : col + TILE]
                dst[:, t : t + TILE] = (fresh * inv[:, col : col + TILE]).astype(BF16)
            send(dst, dst, r_send.at[d, 1, i], r_recv.at[d, 1, i], nbr[d])
            send(dst, dst, p_send.at[d, 1, i], p_recv.at[d, 1, i], partner)

    arrived(nrm.at[1 - c], n_recv)
    nall[y] = nrm[...]
    for d in range(1, 4):
        send(nrm, nall.at[y], y_send.at[d - 1], y_recv.at[d - 1], {"tp": lax.rem(y + d, 4)})

    for h in (2, 3, 4):
        for i, (a, r0, n) in enumerate(CHUNKS):
            for d in range(2):
                if h == 4 and i not in LAST[d]:
                    continue
                dst = place(a, origin(d, h), c, r0, n)
                arrived(dst, r_recv.at[d, h - 1, i])
                if h == 2 or (h == 3 and i in LAST[d]):
                    send(dst, dst, r_send.at[d, h, i], r_recv.at[d, h, i], nbr[d])
                send(dst, dst, p_send.at[d, h, i], p_recv.at[d, h, i], partner)
        if h == 2:
            for d in range(1, 4):
                arrived(nall.at[lax.rem(y - d + 4, 4)], y_recv.at[d - 1])
            for b in range(4):
                for yy in range(4):
                    k = 4 * b + yy
                    for g in range(4):
                        s = 4 * g + b
                        nout[g : g + 1, 40 * k : 40 * k + 40] = nall[yy, s % 2, s // 2 : s // 2 + 1, 0:40]
            for g in range(4):
                for j in range(5):
                    nrow[5 * g + j : 5 * g + j + 1, :] = nout[g : g + 1, 128 * j : 128 * (j + 1)]
            on[...] = nrow[...].astype(BF16)

    for i, (a, r0, n) in enumerate(CHUNKS):
        arrived(place(a, z, 1 - c, r0, n), p_recv.at[0, 0, i])
    for h in (1, 2, 3, 4):
        for i, (a, r0, n) in enumerate(CHUNKS):
            for d in range(2):
                if h == 4 and i not in LAST[d]:
                    continue
                arrived(place(a, z + h * step[d], 1 - c, r0, n), p_recv.at[d, h, i])
    for cp in sends:
        cp.wait_send()


def flush(*refs):
    sem = refs[-1]
    copies = [pltpu.make_async_copy(refs[i], refs[7 + i], sem.at[i]) for i in range(7)]
    for cp in copies:
        cp.start()
    for cp in copies:
        cp.wait()


def per_device(wq, lq, hq, wk, lk, hk, wv, lv, hv, nt, ns):
    rows = wq.shape[0]
    n = len(CHUNKS)
    dma = pltpu.SemaphoreType.DMA
    any_spec = pl.BlockSpec(memory_space=pltpu.HBM)
    vm = pl.BlockSpec(memory_space=pltpu.VMEM)
    widths = (wq.shape[1], wk.shape[1], wv.shape[1])
    rank = hq.shape[0]
    wide = sum(widths)
    out_shape = (
        *(pltpu.VMEM((16 * rows, m), BF16) for m in widths),
        *(pltpu.VMEM((1, m), F32) for m in widths),
        pltpu.VMEM((20, 128), BF16),
    )
    scratch = (
        *(pltpu.VMEM((rows, m), BF16) for m in widths),
        *(pltpu.VMEM((rank, rows), BF16) for _ in widths),
        *(pltpu.VMEM((rank, m), BF16) for m in widths),
        pltpu.VMEM((40,), F32),
        pltpu.VMEM((40,), F32),
        *(pltpu.VMEM((2, rows, m), BF16) for m in widths),
        *(pltpu.VMEM((2, rank, rows), BF16) for _ in widths),
        pltpu.VMEM((3, rows, wide), F32),
        pltpu.VMEM((2, 8, 128), F32),
        pltpu.VMEM((8, 128), F32),
        pltpu.VMEM((8, 128), F32),
        pltpu.VMEM((8, 8, 128), F32),
        pltpu.VMEM((2, 8, 128), F32),
        pltpu.VMEM((2, 8, 128), F32),
        pltpu.VMEM((4, 2, 8, 128), F32),
        pltpu.VMEM((1, wide), F32),
        pltpu.VMEM((4, 640), F32),
        pltpu.VMEM((20, 128), F32),
        dma((11,)),
        dma, dma, dma, dma,
        dma((7,)), dma((7,)),
        dma, dma, dma, dma,
        dma((3,)), dma((3,)),
        dma((2, 3)), dma((2, 3)),
        dma((2, 4, n)), dma((2, 4, n)),
        dma((2, 5, n)), dma((2, 5, n)),
    )
    oq, ok, ov, fq, fk, fv, on = pl.pallas_call(
        kernel,
        out_shape=out_shape,
        in_specs=[any_spec] * 11,
        out_specs=(vm,) * 7,
        scratch_shapes=scratch,
        compiler_params=pltpu.CompilerParams(
            collective_id=0, has_side_effects=True, vmem_limit_bytes=24 * 1024 * 1024
        ),
    )(*(pltpu.with_memory_space_constraint(a, pltpu.HBM) for a in (wq, lq.T, hq, wk, lk.T, hk, wv, lv.T, hv, nt, ns)))
    made = (oq, ok, ov, fq, fk, fv, on)
    oq, ok, ov, fq, fk, fv, on = pl.pallas_call(
        flush,
        out_shape=tuple(jax.ShapeDtypeStruct(a.shape, a.dtype) for a in made),
        in_specs=[vm] * 7,
        out_specs=(pl.BlockSpec(memory_space=pltpu.HBM),) * 7,
        scratch_shapes=(dma((7,)),),
        compiler_params=pltpu.CompilerParams(vmem_limit_bytes=1024 * 1024),
    )(*(pltpu.with_memory_space_constraint(a, pltpu.VMEM) for a in made))
    return oq, ok, ov, fq.reshape(-1), fk.reshape(-1), fv.reshape(-1), on.reshape(-1)


def solution(mesh):
    return jax.shard_map(
        per_device,
        mesh=mesh,
        in_specs=(
            P(("shift", "shard"), "tp"),
            P(("shift", "shard"), None),
            P("shift", "tp"),
            P(("shift", "shard"), "tp"),
            P(("shift", "shard"), None),
            P("shift", "tp"),
            P(("shift", "shard"), "tp"),
            P(("shift", "shard"), None),
            P("shift", "tp"),
            P(("shift", "shard", "tp")),
            P(("shift", "shard", "tp")),
        ),
        out_specs=(
            P("shift", "tp"),
            P("shift", "tp"),
            P("shift", "tp"),
            P(("shift", "tp")),
            P(("shift", "tp")),
            P(("shift", "tp")),
            P("shift"),
        ),
        check_vma=False,
    )
```

```python
import functools

import jax
import jax.numpy as jnp
from jax import lax
from jax.experimental import pallas as pl
from jax.experimental.pallas import tpu as pltpu
from jax.sharding import PartitionSpec as P

MESH = pl.DeviceIdType.MESH
F32 = jnp.float32
BF16 = jnp.bfloat16

mix_rate = 1.0

CHUNKS = ((1, 0, 160), (2, 0, 160), (0, 0, 48), (0, 48, 64), (0, 112, 48))
LAST = ((0, 1, 2), (3, 4))
COLS = (0, 1024, 1280, 1536)
TILE = 256


def kernel(
    wq, lq, hq, wk, lk, hk, wv, lv, hv, nt, ns,
    oq, ok, ov, fq, fk, fv, on,
    sw0, sw1, sw2, low, sh0, sh1, sh2, snt, sns,
    rw0, rw1, rw2, rlow, prod,
    st, stp, msg, gath, fin, nrm, nall, inv, nout, nrow,
    load_sem, far, sr_send, sr_recv, g_send, g_recv, f_send, f_recv,
    n_send, n_recv, y_send, y_recv, low_send, low_recv, ly_send, ly_recv, r_send, r_recv, p_send, p_recv,
):
    shard = lax.axis_index("shard")
    y = lax.axis_index("tp")
    z, c = shard // 2, shard % 2
    nz, ny = 8, 4
    rows = wq.shape[0]
    d_model = rows * 16
    outs = (oq, ok, ov)
    w = (sw0, sw1, sw2)
    high = (sh0, sh1, sh2)
    rw = (rw0, rw1, rw2)
    step = (1 - 2 * c, 2 * c - 1)

    def at(zz, cc):
        return {"shard": lax.rem(zz + 4 * nz, nz) * 2 + cc}

    def rank_of(d):
        return {"tp": lax.rem(y + d, ny)}

    partner = at(z, 1 - c)
    nbr = (at(z + step[0], c), at(z + step[1], c))

    pairs = (
        (lq, low.at[0]), (lk, low.at[1]), (lv, low.at[2]), (wk, sw1), (wv, sw2),
        (hk, sh1), (hv, sh2), (hq, sh0), (wq, sw0), (nt, snt), (ns, sns),
    )
    loads = [pltpu.make_async_copy(src, dst, load_sem.at[i]) for i, (src, dst) in enumerate(pairs)]
    for cp in loads:
        cp.start()

    barrier = pltpu.get_barrier_semaphore()
    peers = [*nbr, partner, *(rank_of(d) for d in range(1, ny))]
    for peer in peers:
        pl.semaphore_signal(barrier, inc=1, device_id=peer, device_id_type=MESH)
    pl.semaphore_wait(barrier, len(peers))

    def pass_on(k):
        for d in range(2):
            pl.semaphore_signal(far.at[d, k - 1], inc=1, device_id=nbr[d], device_id_type=MESH)

    def heard(k):
        for d in range(2):
            pl.semaphore_wait(far.at[d, k - 1], 1)

    pass_on(1)

    sends = []

    def send(src, dst, s_sem, r_sem, to):
        cp = pltpu.make_async_remote_copy(
            src_ref=src, dst_ref=dst, send_sem=s_sem, recv_sem=r_sem, device_id=to, device_id_type=MESH
        )
        cp.start()
        sends.append(cp)

    def arrived(dst, sem):
        pltpu.make_async_remote_copy(
            src_ref=dst, dst_ref=dst, send_sem=sem, recv_sem=sem, device_id=partner, device_id_type=MESH
        ).wait_recv()

    def send_raw(i):
        a, r0, n = CHUNKS[i]
        for d in range(2):
            send(w[a].at[pl.ds(r0, n)], rw[a].at[d, pl.ds(r0, n)], r_send.at[d, 0, i], r_recv.at[d, 0, i], nbr[d])

    def quarter(rank):
        share = low.shape[1] // ny
        return pl.ds(pl.multiple_of(rank * share, share), share)

    for i in range(3):
        loads[i].wait()
    for d in range(2):
        send(low.at[:, quarter(y)], rlow.at[d, :, quarter(y)], low_send.at[d], low_recv.at[d], nbr[d])
    loads[3].wait()
    send_raw(0)
    loads[4].wait()
    send_raw(1)

    def product(l_ref, h_ref, out, a):
        for t in range(0, COLS[a + 1] - COLS[a], TILE):
            out[:, COLS[a] + t : COLS[a] + t + TILE] = mix_rate * lax.dot_general(
                l_ref[...], h_ref[:, t : t + TILE], (((0,), (0,)), ((), ())), preferred_element_type=F32
            )

    for i in range(5, 11):
        loads[i].wait()
    st[...] = jnp.zeros_like(st)
    for a in (1, 2, 0):
        product(low.at[a], high[a], prod.at[2], a)
        for t in range(0, COLS[a + 1] - COLS[a], TILE):
            col = COLS[a] + t
            fresh = w[a][:, t : t + TILE].astype(F32) + prod[2, :, col : col + TILE]
            prod[2, :, col : col + TILE] = fresh
            total = jnp.sum(jnp.abs(fresh), axis=0, keepdims=True)
            for g in range(TILE // 128):
                j = col // 128 + g
                st[j // 6, j % 6 : j % 6 + 1, :] = total[:, 128 * g : 128 * (g + 1)]

    send(st.at[1 - c], stp, sr_send, sr_recv, partner)
    heard(1)
    pass_on(2)
    arrived(stp, sr_recv)
    msg[0:6, :] = st[c, 0:6, :] + stp[0:6, :]
    msg[6:8, :] = jnp.zeros((2, 128), F32)
    msg[6:7, 0:40] = (snt[...] + sns[...]).reshape(1, 40)
    gath[z] = msg[...]

    def send_sums(d):
        send(msg, gath.at[z], g_send.at[d - 1], g_recv.at[d - 1], at(z + d, c))

    for d in (2, nz - 2, 1, nz - 1):
        send_sums(d)
    send_raw(2)
    heard(2)
    pass_on(3)
    for d in (3, nz - 3):
        send_sums(d)
    send_raw(3)
    heard(3)
    send_sums(4)
    send_raw(4)

    for d in range(2):
        mine = rlow.at[d, :, quarter(y)]
        arrived(mine, low_recv.at[d])
        for k in range(1, ny):
            send(mine, mine, ly_send.at[d, k - 1], ly_recv.at[d, k - 1], rank_of(k))
    for d in range(2):
        for k in range(1, ny):
            arrived(rlow.at[d, :, quarter(lax.rem(y - k + ny, ny))], ly_recv.at[d, k - 1])
        for a in range(3):
            product(rlow.at[d, a], high[a], prod.at[d], a)

    for d in range(1, nz):
        arrived(gath.at[lax.rem(z - d + nz, nz)], g_recv.at[d - 1])
    total = gath[0]
    for k in range(1, nz):
        total = total + gath[k]
    fin[c] = total * (1.0 / d_model)
    send(fin.at[c], fin.at[c], f_send, f_recv, partner)
    for k in range(nz):
        nrm[c, k : k + 1, :] = gath[k, 6:7, :]
    send(nrm.at[c], nrm.at[c], n_send, n_recv, partner)
    arrived(fin.at[1 - c], f_recv)
    for j in range(12):
        row = fin[j // 6, j % 6 : j % 6 + 1, :]
        inv[:, 128 * j : 128 * (j + 1)] = 1.0 / row
        if j < 8:
            fq[:, 128 * j : 128 * (j + 1)] = row
        elif j < 10:
            fk[:, 128 * (j - 8) : 128 * (j - 7)] = row
        else:
            fv[:, 128 * (j - 10) : 128 * (j - 9)] = row

    def place(a, zz, cc, r0, n):
        first = pl.multiple_of((lax.rem(zz + 4 * nz, nz) * 2 + cc) * rows, 16)
        return outs[a].at[pl.ds(first + r0, n)]

    def origin(d, h):
        return z - h * step[d]

    for i, (a, r0, n) in enumerate(CHUNKS):
        for d in range(2):
            arrived(rw[a].at[d, pl.ds(r0, n)], r_recv.at[d, 0, i])
            dst = place(a, origin(d, 1), c, r0, n)
            for t in range(0, COLS[a + 1] - COLS[a], TILE):
                col = COLS[a] + t
                fresh = rw[a][d, r0 : r0 + n, t : t + TILE].astype(F32) + prod[d, r0 : r0 + n, col : col + TILE]
                dst[:, t : t + TILE] = (fresh * inv[:, col : col + TILE]).astype(BF16)
            send(dst, dst, r_send.at[d, 1, i], r_recv.at[d, 1, i], nbr[d])
            send(dst, dst, p_send.at[d, 1, i], p_recv.at[d, 1, i], partner)
    for i, (a, r0, n) in enumerate(CHUNKS):
        dst = place(a, z, c, r0, n)
        for t in range(0, COLS[a + 1] - COLS[a], TILE):
            col = COLS[a] + t
            dst[:, t : t + TILE] = (prod[2, r0 : r0 + n, col : col + TILE] * inv[:, col : col + TILE]).astype(BF16)
        send(dst, dst, p_send.at[0, 0, i], p_recv.at[0, 0, i], partner)

    arrived(nrm.at[1 - c], n_recv)
    nall[y] = nrm[...]
    for d in range(1, ny):
        send(nrm, nall.at[y], y_send.at[d - 1], y_recv.at[d - 1], rank_of(d))

    for h in (2, 3, 4):
        for i, (a, r0, n) in enumerate(CHUNKS):
            for d in range(2):
                if h == 4 and i not in LAST[d]:
                    continue
                dst = place(a, origin(d, h), c, r0, n)
                arrived(dst, r_recv.at[d, h - 1, i])
                if h == 2 or (h == 3 and i in LAST[d]):
                    send(dst, dst, r_send.at[d, h, i], r_recv.at[d, h, i], nbr[d])
                send(dst, dst, p_send.at[d, h, i], p_recv.at[d, h, i], partner)
        if h == 2:
            for d in range(1, ny):
                arrived(nall.at[lax.rem(y - d + ny, ny)], y_recv.at[d - 1])
            for b in range(4):
                for yy in range(ny):
                    k = 4 * b + yy
                    for g in range(4):
                        s = 4 * g + b
                        nout[g : g + 1, 40 * k : 40 * k + 40] = nall[yy, s % 2, s // 2 : s // 2 + 1, 0:40]
            for g in range(4):
                for j in range(5):
                    nrow[5 * g + j : 5 * g + j + 1, :] = nout[g : g + 1, 128 * j : 128 * (j + 1)]
            on[...] = nrow[...].astype(BF16)

    for i, (a, r0, n) in enumerate(CHUNKS):
        arrived(place(a, z, 1 - c, r0, n), p_recv.at[0, 0, i])
    for h in (1, 2, 3, 4):
        for i, (a, r0, n) in enumerate(CHUNKS):
            for d in range(2):
                if h == 4 and i not in LAST[d]:
                    continue
                arrived(place(a, z + h * step[d], 1 - c, r0, n), p_recv.at[d, h, i])
    for cp in sends:
        cp.wait_send()


def flush(*refs):
    sem = refs[-1]
    pairs = [(refs[i], refs[7 + i]) for i in range(1, 7)]
    n = refs[0].shape[0] // 4
    pairs = [(refs[0].at[pl.ds(k * n, n)], refs[7].at[pl.ds(k * n, n)]) for k in range(4)] + pairs
    copies = [pltpu.make_async_copy(src, dst, sem.at[i]) for i, (src, dst) in enumerate(pairs)]
    for cp in copies:
        cp.start()
    for cp in copies:
        cp.wait()


def per_device(wq, lq, hq, wk, lk, hk, wv, lv, hv, nt, ns):
    rows = wq.shape[0]
    n = len(CHUNKS)
    dma = pltpu.SemaphoreType.DMA
    any_spec = pl.BlockSpec(memory_space=pltpu.HBM)
    vm = pl.BlockSpec(memory_space=pltpu.VMEM)
    widths = (wq.shape[1], wk.shape[1], wv.shape[1])
    rank = hq.shape[0]
    wide = sum(widths)
    out_shape = (
        *(pltpu.VMEM((16 * rows, m), BF16) for m in widths),
        *(pltpu.VMEM((1, m), F32) for m in widths),
        pltpu.VMEM((20, 128), BF16),
    )
    scratch = (
        *(pltpu.VMEM((rows, m), BF16) for m in widths),
        pltpu.VMEM((3, rank, rows), BF16),
        *(pltpu.VMEM((rank, m), BF16) for m in widths),
        pltpu.VMEM((40,), F32),
        pltpu.VMEM((40,), F32),
        *(pltpu.VMEM((2, rows, m), BF16) for m in widths),
        pltpu.VMEM((2, 3, rank, rows), BF16),
        pltpu.VMEM((3, rows, wide), F32),
        pltpu.VMEM((2, 8, 128), F32),
        pltpu.VMEM((8, 128), F32),
        pltpu.VMEM((8, 128), F32),
        pltpu.VMEM((8, 8, 128), F32),
        pltpu.VMEM((2, 8, 128), F32),
        pltpu.VMEM((2, 8, 128), F32),
        pltpu.VMEM((4, 2, 8, 128), F32),
        pltpu.VMEM((1, wide), F32),
        pltpu.VMEM((4, 640), F32),
        pltpu.VMEM((20, 128), F32),
        dma((11,)),
        pltpu.SemaphoreType.REGULAR((2, 3)),
        dma, dma,
        dma((7,)), dma((7,)),
        dma, dma, dma, dma,
        dma((3,)), dma((3,)),
        dma((2,)), dma((2,)),
        dma((2, 3)), dma((2, 3)),
        dma((2, 4, n)), dma((2, 4, n)),
        dma((2, 5, n)), dma((2, 5, n)),
    )
    oq, ok, ov, fq, fk, fv, on = pl.pallas_call(
        kernel,
        out_shape=out_shape,
        in_specs=[any_spec] * 11,
        out_specs=(vm,) * 7,
        scratch_shapes=scratch,
        compiler_params=pltpu.CompilerParams(
            collective_id=0, has_side_effects=True, vmem_limit_bytes=24 * 1024 * 1024
        ),
    )(*(pltpu.with_memory_space_constraint(a, pltpu.HBM) for a in (wq, lq.T, hq, wk, lk.T, hk, wv, lv.T, hv, nt, ns)))
    made = (oq, ok, ov, fq, fk, fv, on)
    oq, ok, ov, fq, fk, fv, on = pl.pallas_call(
        flush,
        out_shape=tuple(jax.ShapeDtypeStruct(a.shape, a.dtype) for a in made),
        in_specs=[vm] * 7,
        out_specs=(pl.BlockSpec(memory_space=pltpu.HBM),) * 7,
        scratch_shapes=(dma((10,)),),
        compiler_params=pltpu.CompilerParams(vmem_limit_bytes=1024 * 1024),
    )(*(pltpu.with_memory_space_constraint(a, pltpu.VMEM) for a in made))
    return oq, ok, ov, fq.reshape(-1), fk.reshape(-1), fv.reshape(-1), on.reshape(-1)


def solution(mesh):
    return jax.shard_map(
        per_device,
        mesh=mesh,
        in_specs=(
            P(("shift", "shard"), "tp"),
            P(("shift", "shard"), None),
            P("shift", "tp"),
            P(("shift", "shard"), "tp"),
            P(("shift", "shard"), None),
            P("shift", "tp"),
            P(("shift", "shard"), "tp"),
            P(("shift", "shard"), None),
            P("shift", "tp"),
            P(("shift", "shard", "tp")),
            P(("shift", "shard", "tp")),
        ),
        out_specs=(
            P("shift", "tp"),
            P("shift", "tp"),
            P("shift", "tp"),
            P(("shift", "tp")),
            P(("shift", "tp")),
            P(("shift", "tp")),
            P("shift"),
        ),
        check_vma=False,
    )
```

```python
import functools

import jax
import jax.numpy as jnp
from jax import lax
from jax.experimental import pallas as pl
from jax.experimental.pallas import tpu as pltpu
from jax.sharding import PartitionSpec as P

MESH = pl.DeviceIdType.MESH
F32 = jnp.float32
BF16 = jnp.bfloat16

mix_rate = 1.0

RAW = ((0, 48), (48, 32), (80, 80))
EARLY = 1
HOP = ((0, 80), (80, 80))
LAST = ((0,), (1,))
TILE = 256
HALF = 6


def kernel(
    wq, lq, hq, wk, lk, hk, wv, lv, hv, nt, ns,
    out, fq, fk, fv, on,
    own, low, high, snt, sns, raw, rlow, prod, st, stp, msg, gath, fin, nall, inv, nout, nrow,
    load_sem, near, far, ranks, st_send, st_recv, g_send, g_recv, f_send, f_recv, y_send, y_recv, on_send, on_recv,
    low_send, low_recv, ly_send, ly_recv, raw_send, raw_recv, r_send, r_recv, p_send, p_recv,
):
    shard = lax.axis_index("shard")
    y = lax.axis_index("tp")
    z, c = shard // 2, shard % 2
    nz, ny = 8, 4
    rows, wide = own.shape
    d_model = rows * 16
    step = (1 - 2 * c, 2 * c - 1)

    def at(zz, cc):
        return {"shard": lax.rem(zz + 4 * nz, nz) * 2 + cc}

    def rank_of(d):
        return {"tp": lax.rem(y + d, ny)}

    partner = at(z, 1 - c)
    nbr = (at(z + step[0], c), at(z + step[1], c))

    nq, nk = wq.shape[1], wk.shape[1]
    parts = (pl.ds(0, nq), pl.ds(nq, nk), pl.ds(nq + nk, nk))
    pairs = (
        (lq, low.at[0]), (lk, low.at[1]), (lv, low.at[2]),
        (wq, own.at[:, parts[0]]), (wk, own.at[:, parts[1]]), (wv, own.at[:, parts[2]]),
        (hq, high.at[:, parts[0]]), (hk, high.at[:, parts[1]]), (hv, high.at[:, parts[2]]),
        (nt, snt), (ns, sns),
    )
    loads = [pltpu.make_async_copy(src, dst, load_sem.at[i]) for i, (src, dst) in enumerate(pairs)]
    for cp in loads:
        cp.start()

    barrier = pltpu.get_barrier_semaphore()

    def signal(sem, to):
        pl.semaphore_signal(sem, inc=1, device_id=to, device_id_type=MESH)

    for peer in (at(z - 1, 0), at(z + 1, 0)):
        signal(barrier, peer)

    @pl.when(c == 1)
    def _():
        signal(barrier, partner)

    @pl.when(c == 0)
    def _():
        pl.semaphore_wait(barrier, 5)
        signal(near, partner)

    @pl.when(c == 1)
    def _():
        pl.semaphore_wait(near, 1)
        for d in range(1, ny):
            signal(barrier, rank_of(d))

    def pass_on(k):
        for d in range(2):
            signal(far.at[d, k - 1], nbr[d])

    def heard(k):
        for d in range(2):
            pl.semaphore_wait(far.at[d, k - 1], 1)

    pass_on(1)

    sends = []

    def send(src, dst, s_sem, r_sem, to):
        cp = pltpu.make_async_remote_copy(
            src_ref=src, dst_ref=dst, send_sem=s_sem, recv_sem=r_sem, device_id=to, device_id_type=MESH
        )
        cp.start()
        sends.append(cp)

    def arrived(dst, sem):
        pltpu.make_async_remote_copy(
            src_ref=dst, dst_ref=dst, send_sem=sem, recv_sem=sem, device_id=partner, device_id_type=MESH
        ).wait_recv()

    def send_raw(i):
        piece = pl.ds(*RAW[i])
        for d in range(2):
            send(own.at[piece], raw.at[d, piece], raw_send.at[d, i], raw_recv.at[d, i], nbr[d])

    def quarter(rank):
        share = low.shape[1] // ny
        return pl.ds(pl.multiple_of(rank * share, share), share)

    for i in range(3):
        loads[i].wait()
    for d in range(2):
        send(low.at[:, quarter(y)], rlow.at[d, :, quarter(y)], low_send.at[d], low_recv.at[d], nbr[d])
    for i in range(3, 6):
        loads[i].wait()
    for i in range(EARLY):
        send_raw(i)
    for i in range(6, 11):
        loads[i].wait()

    def array_of(col):
        return 0 if col < nq else 1 if col < nq + nk else 2

    def product(l_ref, col):
        return mix_rate * lax.dot_general(
            l_ref[array_of(col)], high[:, col : col + TILE], (((0,), (0,)), ((), ())), preferred_element_type=F32
        )

    for col in range(0, wide, TILE):
        fresh = own[:, col : col + TILE].astype(F32) + product(low, col)
        prod[2, :, col : col + TILE] = fresh
        total = jnp.sum(jnp.abs(fresh), axis=0, keepdims=True)
        for g in range(TILE // 128):
            j = col // 128 + g
            st[j // HALF, j % HALF] = total[:, 128 * g : 128 * (g + 1)]
    send(st.at[1 - c], stp, st_send, st_recv, partner)
    heard(1)
    pass_on(2)
    msg[HALF] = jnp.zeros((1, 128), F32)
    msg[HALF, 0:1, 0:40] = (snt[...] + sns[...]).reshape(1, 40)
    arrived(stp, st_recv)
    msg[0:HALF] = st[c] + stp[...]
    gath[z] = msg[...]

    def send_sums(d):
        send(msg, gath.at[z], g_send.at[d - 1], g_recv.at[d - 1], at(z + d, c))

    for d in (2, nz - 2, 1, nz - 1):
        send_sums(d)
    heard(2)
    pass_on(3)
    for d in (3, nz - 3):
        send_sums(d)
    heard(3)
    send_sums(4)
    for i in range(EARLY, len(RAW)):
        send_raw(i)

    @pl.when(c == 1)
    def _():
        pl.semaphore_wait(barrier, ny - 1)
        signal(ranks, partner)

    @pl.when(c == 0)
    def _():
        pl.semaphore_wait(ranks, 1)

    for d in range(2):
        mine = rlow.at[d, :, quarter(y)]
        arrived(mine, low_recv.at[d])
        for k in range(1, ny):
            send(mine, mine, ly_send.at[d, k - 1], ly_recv.at[d, k - 1], rank_of(k))
    for d in range(2):
        for k in range(1, ny):
            arrived(rlow.at[d, :, quarter(lax.rem(y - k + ny, ny))], ly_recv.at[d, k - 1])
        for col in range(0, wide, TILE):
            prod[d, :, col : col + TILE] = product(rlow.at[d], col)

    for d in range(1, nz):
        arrived(gath.at[lax.rem(z - d + nz, nz)], g_recv.at[d - 1])
    total = gath[0, 0:HALF]
    for k in range(1, nz):
        total = total + gath[k, 0:HALF]
    fin[c, 0:HALF] = total * (1.0 / d_model)
    for k in range(nz):
        fin[c, HALF + k] = gath[k, HALF]
    send(fin.at[c], fin.at[c], f_send, f_recv, partner)
    arrived(fin.at[1 - c], f_recv)
    for j in range(2 * HALF):
        factor = fin[j // HALF, j % HALF]
        inv[:, 128 * j : 128 * (j + 1)] = 1.0 / factor
        if j < 8:
            fq[:, 128 * j : 128 * (j + 1)] = factor
        elif j < 10:
            fk[:, 128 * (j - 8) : 128 * (j - 7)] = factor
        else:
            fv[:, 128 * (j - 10) : 128 * (j - 9)] = factor

    def place(zz, cc, piece):
        first = pl.multiple_of((lax.rem(zz + 4 * nz, nz) * 2 + cc) * rows, 16)
        return out.at[pl.ds(first + piece[0], piece[1])]

    def origin(d, h):
        return z - h * step[d]

    def to_partner(d, h, i):
        dst = place(origin(d, h), c, HOP[i])
        send(dst, dst, p_send.at[d, h, i], p_recv.at[d, h, i], partner)

    def onward(d, h, i):
        dst = place(origin(d, h), c, HOP[i])
        send(dst, dst, r_send.at[d, h, i], r_recv.at[d, h, i], nbr[d])

    for i, (h0, hn) in enumerate(HOP):
        for d in range(2):
            for j, (r0, n) in enumerate(RAW):
                if not h0 <= r0 < h0 + hn:
                    continue
                arrived(raw.at[d, pl.ds(r0, n)], raw_recv.at[d, j])
                dst = place(origin(d, 1), c, (r0, n))
                for col in range(0, wide, TILE):
                    fresh = raw[d, r0 : r0 + n, col : col + TILE].astype(F32) + prod[d, r0 : r0 + n, col : col + TILE]
                    dst[:, col : col + TILE] = (fresh * inv[:, col : col + TILE]).astype(BF16)
            onward(d, 1, i)
            to_partner(d, 1, i)
    dst = place(z, c, (0, rows))
    for col in range(0, wide, TILE):
        dst[:, col : col + TILE] = (prod[2, :, col : col + TILE] * inv[:, col : col + TILE]).astype(BF16)
    send(dst, dst, p_send.at[0, 0, 0], p_recv.at[0, 0, 0], partner)

    gains = fin.at[:, pl.ds(HALF, nz)]
    to_ranks = [
        pltpu.make_async_remote_copy(
            src_ref=gains, dst_ref=nall.at[y], send_sem=y_send.at[d - 1], recv_sem=y_recv.at[d - 1],
            device_id=rank_of(d), device_id_type=MESH,
        )
        for d in range(1, ny)
    ]
    to_core0 = pltpu.make_async_remote_copy(
        src_ref=on, dst_ref=on, send_sem=on_send, recv_sem=on_recv, device_id=partner, device_id_type=MESH
    )

    @pl.when(c == 1)
    def _():
        for cp in to_ranks:
            cp.start()
        nall[y] = fin[:, HALF : HALF + nz]

    for h in (2, 3, 4):
        for i in range(len(HOP)):
            for d in range(2):
                if h == 4 and i not in LAST[d]:
                    continue
                arrived(place(origin(d, h), c, HOP[i]), r_recv.at[d, h - 1, i])
                if h == 2 or (h == 3 and i in LAST[d]):
                    onward(d, h, i)
                to_partner(d, h, i)
        if h == 2:

            @pl.when(c == 1)
            def _():
                for d in range(1, ny):
                    arrived(nall.at[lax.rem(y - d + ny, ny)], y_recv.at[d - 1])
                for b in range(4):
                    for yy in range(ny):
                        k = 4 * b + yy
                        for g in range(4):
                            s = 4 * g + b
                            nout[g : g + 1, 40 * k : 40 * k + 40] = nall[yy, s % 2, s // 2, :, 0:40]
                for g in range(4):
                    for j in range(5):
                        nrow[5 * g + j : 5 * g + j + 1, :] = nout[g : g + 1, 128 * j : 128 * (j + 1)]
                on[...] = nrow[...].astype(BF16)
                to_core0.start()

    arrived(place(z, 1 - c, (0, rows)), p_recv.at[0, 0, 0])
    for h in (1, 2, 3, 4):
        for i in range(len(HOP)):
            for d in range(2):
                if h == 4 and i not in LAST[d]:
                    continue
                arrived(place(z + h * step[d], 1 - c, HOP[i]), p_recv.at[d, h, i])
    for cp in sends:
        cp.wait_send()

    @pl.when(c == 1)
    def _():
        for cp in (*to_ranks, to_core0):
            cp.wait_send()

    @pl.when(c == 0)
    def _():
        to_core0.wait_recv()


def flush(out, fq, fk, fv, on, oq, ok, ov, gq, gk, gv, gn, sem):
    nq, nk = oq.shape[1], ok.shape[1]
    n = out.shape[0] // 4
    pairs = [(fq, gq), (fk, gk), (fv, gv), (on, gn)]
    for k in range(4):
        piece = pl.ds(k * n, n)
        for dst, first, m in ((oq, 0, nq), (ok, nq, nk), (ov, nq + nk, nk)):
            pairs.append((out.at[piece, pl.ds(first, m)], dst.at[piece]))
    copies = [pltpu.make_async_copy(src, dst, sem.at[i]) for i, (src, dst) in enumerate(pairs)]
    for cp in copies:
        cp.start()
    for cp in copies:
        cp.wait()


def per_device(wq, lq, hq, wk, lk, hk, wv, lv, hv, nt, ns):
    rows = wq.shape[0]
    dma = pltpu.SemaphoreType.DMA
    hbm = pl.BlockSpec(memory_space=pltpu.HBM)
    vm = pl.BlockSpec(memory_space=pltpu.VMEM)
    widths = (wq.shape[1], wk.shape[1], wv.shape[1])
    rank = hq.shape[0]
    wide = sum(widths)
    out_shape = (
        pltpu.VMEM((16 * rows, wide), BF16),
        *(pltpu.VMEM((1, m), F32) for m in widths),
        pltpu.VMEM((20, 128), BF16),
    )
    scratch = (
        pltpu.VMEM((rows, wide), BF16),
        pltpu.VMEM((3, rank, rows), BF16),
        pltpu.VMEM((rank, wide), BF16),
        pltpu.VMEM((40,), F32),
        pltpu.VMEM((40,), F32),
        pltpu.VMEM((2, rows, wide), BF16),
        pltpu.VMEM((2, 3, rank, rows), BF16),
        pltpu.VMEM((3, rows, wide), F32),
        pltpu.VMEM((2, HALF, 1, 128), F32),
        pltpu.VMEM((HALF, 1, 128), F32),
        pltpu.VMEM((HALF + 1, 1, 128), F32),
        pltpu.VMEM((8, HALF + 1, 1, 128), F32),
        pltpu.VMEM((2, HALF + 8, 1, 128), F32),
        pltpu.VMEM((4, 2, 8, 1, 128), F32),
        pltpu.VMEM((1, wide), F32),
        pltpu.VMEM((4, 640), F32),
        pltpu.VMEM((20, 128), F32),
        dma((11,)),
        pltpu.SemaphoreType.REGULAR,
        pltpu.SemaphoreType.REGULAR((2, 3)),
        pltpu.SemaphoreType.REGULAR,
        dma, dma,
        dma((7,)), dma((7,)),
        dma, dma,
        dma((3,)), dma((3,)),
        dma, dma,
        dma((2,)), dma((2,)),
        dma((2, 3)), dma((2, 3)),
        dma((2, len(RAW))), dma((2, len(RAW))),
        dma((2, 4, len(HOP))), dma((2, 4, len(HOP))),
        dma((2, 5, len(HOP))), dma((2, 5, len(HOP))),
    )
    made = pl.pallas_call(
        kernel,
        out_shape=out_shape,
        in_specs=[hbm] * 11,
        out_specs=(vm,) * 5,
        scratch_shapes=scratch,
        compiler_params=pltpu.CompilerParams(
            collective_id=0, has_side_effects=True, vmem_limit_bytes=24 * 1024 * 1024
        ),
    )(*(pltpu.with_memory_space_constraint(a, pltpu.HBM) for a in (wq, lq.T, hq, wk, lk.T, hk, wv, lv.T, hv, nt, ns)))
    oq, ok, ov, fq, fk, fv, on = pl.pallas_call(
        flush,
        out_shape=(
            *(jax.ShapeDtypeStruct((16 * rows, m), BF16) for m in widths),
            *(jax.ShapeDtypeStruct((1, m), F32) for m in widths),
            jax.ShapeDtypeStruct((20, 128), BF16),
        ),
        in_specs=[vm] * 5,
        out_specs=(hbm,) * 7,
        scratch_shapes=(dma((16,)),),
        compiler_params=pltpu.CompilerParams(vmem_limit_bytes=1024 * 1024),
    )(*(pltpu.with_memory_space_constraint(a, pltpu.VMEM) for a in made))
    return oq, ok, ov, fq.reshape(-1), fk.reshape(-1), fv.reshape(-1), on.reshape(-1)


def solution(mesh):
    return jax.shard_map(
        per_device,
        mesh=mesh,
        in_specs=(
            P(("shift", "shard"), "tp"),
            P(("shift", "shard"), None),
            P("shift", "tp"),
            P(("shift", "shard"), "tp"),
            P(("shift", "shard"), None),
            P("shift", "tp"),
            P(("shift", "shard"), "tp"),
            P(("shift", "shard"), None),
            P("shift", "tp"),
            P(("shift", "shard", "tp")),
            P(("shift", "shard", "tp")),
        ),
        out_specs=(
            P("shift", "tp"),
            P("shift", "tp"),
            P("shift", "tp"),
            P(("shift", "tp")),
            P(("shift", "tp")),
            P(("shift", "tp")),
            P("shift"),
        ),
        check_vma=False,
    )
```

```python
import functools

import jax
import jax.numpy as jnp
from jax import lax
from jax.experimental import pallas as pl
from jax.experimental.pallas import tpu as pltpu
from jax.sharding import PartitionSpec as P

MESH = pl.DeviceIdType.MESH
F32 = jnp.float32
BF16 = jnp.bfloat16

mix_rate = 1.0

RAW = (((0, 80), (80, 80)),) * 2
HOP = ((0, 80), (80, 80))
LAST = ((0,), (1,))
TILE = 256
GROUPS = 12


def kernel(
    wq, lq, hq, wk, lk, hk, wv, lv, hv, nt, ns,
    out, fq, fk, fv, on,
    own, low, high, snt, sns, raw, rlow, prod, st, stp, sums, gains, nall, inv, nout, nrow,
    load_sem, near, far, ranks, st_send, st_recv, g_send, g_recv, f_send, f_recv, y_send, y_recv, on_send, on_recv,
    low_send, low_recv, ly_send, ly_recv, raw_send, raw_recv, r_send, r_recv, p_send, p_recv,
):
    shard = lax.axis_index("shard")
    y = lax.axis_index("tp")
    z, c = shard // 2, shard % 2
    nz, ny = 8, 4
    rows, wide = own.shape
    d_model = rows * 16
    step = (1 - 2 * c, 2 * c - 1)

    def at(zz, cc):
        return {"shard": lax.rem(zz + 4 * nz, nz) * 2 + cc}

    def rank_of(d):
        return {"tp": lax.rem(y + d, ny)}

    partner = at(z, 1 - c)
    nbr = (at(z + step[0], c), at(z + step[1], c))

    nq, nk = wq.shape[1], wk.shape[1]
    parts = (pl.ds(0, nq), pl.ds(nq, nk), pl.ds(nq + nk, nk))
    pairs = (
        (lq, low.at[0]), (lk, low.at[1]), (lv, low.at[2]),
        (wq, own.at[:, parts[0]]), (wk, own.at[:, parts[1]]), (wv, own.at[:, parts[2]]),
        (hq, high.at[:, parts[0]]), (hk, high.at[:, parts[1]]), (hv, high.at[:, parts[2]]),
        (nt, snt), (ns, sns),
    )
    loads = [pltpu.make_async_copy(src, dst, load_sem.at[i]) for i, (src, dst) in enumerate(pairs)]
    for cp in loads:
        cp.start()

    barrier = pltpu.get_barrier_semaphore()

    def signal(sem, to):
        pl.semaphore_signal(sem, inc=1, device_id=to, device_id_type=MESH)

    for peer in (at(z - 1, 1), at(z + 1, 1)):
        signal(barrier, peer)

    @pl.when(c == 0)
    def _():
        signal(barrier, partner)

    @pl.when(c == 1)
    def _():
        pl.semaphore_wait(barrier, 5)
        signal(near, partner)

    @pl.when(c == 0)
    def _():
        pl.semaphore_wait(near, 1)
        for d in range(1, ny):
            signal(barrier, rank_of(d))

    def pass_on(k):
        signal(far.at[k - 1], nbr[0])

    def heard(k):
        pl.semaphore_wait(far.at[k - 1], 1)

    pass_on(1)

    sends = []

    def send(src, dst, s_sem, r_sem, to):
        cp = pltpu.make_async_remote_copy(
            src_ref=src, dst_ref=dst, send_sem=s_sem, recv_sem=r_sem, device_id=to, device_id_type=MESH
        )
        cp.start()
        sends.append(cp)

    def arrived(dst, sem):
        pltpu.make_async_remote_copy(
            src_ref=dst, dst_ref=dst, send_sem=sem, recv_sem=sem, device_id=partner, device_id_type=MESH
        ).wait_recv()

    def send_raw(d, i):
        piece = pl.ds(*RAW[d][i])
        send(own.at[piece], raw.at[d, piece], raw_send.at[d, i], raw_recv.at[d, i], nbr[d])

    def quarter(rank):
        share = low.shape[1] // ny
        return pl.ds(pl.multiple_of(rank * share, share), share)

    for i in range(3):
        loads[i].wait()
    for d in range(2):
        send(low.at[:, quarter(y)], rlow.at[d, :, quarter(y)], low_send.at[d], low_recv.at[d], nbr[d])
    for i in range(3, 6):
        loads[i].wait()
    for d in range(2):
        send_raw(d, 0)
    for i in range(6, 11):
        loads[i].wait()

    def array_of(col):
        return 0 if col < nq else 1 if col < nq + nk else 2

    def product(l_ref, col):
        return mix_rate * lax.dot_general(
            l_ref[array_of(col)], high[:, col : col + TILE], (((0,), (0,)), ((), ())), preferred_element_type=F32
        )

    for col in range(0, wide, TILE):
        fresh = own[:, col : col + TILE].astype(F32) + product(low, col)
        prod[2, :, col : col + TILE] = fresh
        total = jnp.sum(jnp.abs(fresh), axis=0, keepdims=True)
        for g in range(TILE // 128):
            j = col // 128 + g
            st[j] = total[:, 128 * g : 128 * (g + 1)]
    st[GROUPS] = jnp.zeros((1, 128), F32)
    st[GROUPS, 0:1, 0:40] = (snt[...] + sns[...]).reshape(1, 40)
    send(st, stp, st_send, st_recv, partner)
    heard(1)
    pass_on(2)
    arrived(stp, st_recv)
    sums[0, 0:GROUPS] = st[0:GROUPS] + stp[0:GROUPS]
    sums[0, GROUPS + c] = st[GROUPS]
    sums[0, GROUPS + 1 - c] = stp[GROUPS]

    def slot(k):
        return k + c * (nz - 2 * k)

    def chips_sums(k):
        return pltpu.make_async_remote_copy(
            src_ref=sums.at[0], dst_ref=sums.at[slot(k)], send_sem=g_send.at[k - 1], recv_sem=g_recv.at[k - 1],
            device_id=at(z + k * step[1], c), device_id_type=MESH,
        )

    for k in (1, 2):
        chips_sums(k).start()
    heard(2)
    pass_on(3)
    chips_sums(3).start()
    heard(3)

    @pl.when(c == 1)
    def _():
        chips_sums(4).start()

    for i in range(1, len(RAW[1])):
        for d in range(2):
            send_raw(d, i)

    @pl.when(c == 0)
    def _():
        pl.semaphore_wait(barrier, ny - 1)
        signal(ranks, partner)

    @pl.when(c == 1)
    def _():
        pl.semaphore_wait(ranks, 1)

    for d in range(2):
        mine = rlow.at[d, :, quarter(y)]
        arrived(mine, low_recv.at[d])
        for k in range(1, ny):
            send(mine, mine, ly_send.at[d, k - 1], ly_recv.at[d, k - 1], rank_of(k))
    for d in range(2):
        for k in range(1, ny):
            arrived(rlow.at[d, :, quarter(lax.rem(y - k + ny, ny))], ly_recv.at[d, k - 1])
        for col in range(0, wide, TILE):
            prod[d, :, col : col + TILE] = product(rlow.at[d], col)

    def swap(first, n):
        part = sums.at[pl.ds(first, n)]
        return pltpu.make_async_remote_copy(
            src_ref=part, dst_ref=part, send_sem=f_send, recv_sem=f_recv, device_id=partner, device_id_type=MESH
        )

    for k in (1, 2, 3):
        chips_sums(k).wait_recv()

    @pl.when(c == 0)
    def _():
        swap(1, 3).start()
        swap(4, 4).wait_recv()

    @pl.when(c == 1)
    def _():
        chips_sums(4).wait_recv()
        swap(4, 4).start()
        swap(1, 3).wait_recv()

    total = sums[lax.rem(nz - z, nz), 0:GROUPS]
    for k in range(1, nz):
        total = total + sums[lax.rem(k - z + nz, nz), 0:GROUPS]
    total = total * (1.0 / d_model)
    for j in range(GROUPS):
        factor = total[j]
        inv[:, 128 * j : 128 * (j + 1)] = 1.0 / factor
        if j < 8:
            fq[:, 128 * j : 128 * (j + 1)] = factor
        elif j < 10:
            fk[:, 128 * (j - 8) : 128 * (j - 7)] = factor
        else:
            fv[:, 128 * (j - 10) : 128 * (j - 9)] = factor

    def place(zz, cc, piece):
        first = pl.multiple_of((lax.rem(zz + 4 * nz, nz) * 2 + cc) * rows, 16)
        return out.at[pl.ds(first + piece[0], piece[1])]

    def origin(d, h):
        return z - h * step[d]

    def to_partner(d, h, i):
        dst = place(origin(d, h), c, HOP[i])
        send(dst, dst, p_send.at[d, h, i], p_recv.at[d, h, i], partner)

    def onward(d, h, i):
        dst = place(origin(d, h), c, HOP[i])
        send(dst, dst, r_send.at[d, h, i], r_recv.at[d, h, i], nbr[d])

    for i, (h0, hn) in enumerate(HOP):
        for d in range(2):
            for j, (r0, n) in enumerate(RAW[d]):
                if not h0 <= r0 < h0 + hn:
                    continue
                arrived(raw.at[d, pl.ds(r0, n)], raw_recv.at[d, j])
                dst = place(origin(d, 1), c, (r0, n))
                for col in range(0, wide, TILE):
                    fresh = raw[d, r0 : r0 + n, col : col + TILE].astype(F32) + prod[d, r0 : r0 + n, col : col + TILE]
                    dst[:, col : col + TILE] = (fresh * inv[:, col : col + TILE]).astype(BF16)
            onward(d, 1, i)
            to_partner(d, 1, i)
    dst = place(z, c, (0, rows))
    for col in range(0, wide, TILE):
        dst[:, col : col + TILE] = (prod[2, :, col : col + TILE] * inv[:, col : col + TILE]).astype(BF16)
    send(dst, dst, p_send.at[0, 0, 0], p_recv.at[0, 0, 0], partner)

    to_ranks = [
        pltpu.make_async_remote_copy(
            src_ref=gains, dst_ref=nall.at[y], send_sem=y_send.at[d - 1], recv_sem=y_recv.at[d - 1],
            device_id=rank_of(d), device_id_type=MESH,
        )
        for d in range(1, ny)
    ]
    to_partner_norm = pltpu.make_async_remote_copy(
        src_ref=on, dst_ref=on, send_sem=on_send, recv_sem=on_recv, device_id=partner, device_id_type=MESH
    )

    @pl.when(c == 0)
    def _():
        for k in range(nz):
            gains[k] = sums[lax.rem(k - z + nz, nz), GROUPS : GROUPS + 2]
        nall[y] = gains[...]
        for cp in to_ranks:
            cp.start()

    for h in (2, 3, 4):
        for i in range(len(HOP)):
            for d in range(2):
                if h == 4 and i not in LAST[d]:
                    continue
                arrived(place(origin(d, h), c, HOP[i]), r_recv.at[d, h - 1, i])
                if h == 2 or (h == 3 and i in LAST[d]):
                    onward(d, h, i)
                to_partner(d, h, i)
        if h == 2:

            @pl.when(c == 0)
            def _():
                for d in range(1, ny):
                    arrived(nall.at[lax.rem(y - d + ny, ny)], y_recv.at[d - 1])
                for b in range(4):
                    for yy in range(ny):
                        k = 4 * b + yy
                        for g in range(4):
                            s = 4 * g + b
                            nout[g : g + 1, 40 * k : 40 * k + 40] = nall[yy, s // 2, s % 2, :, 0:40]
                for g in range(4):
                    for j in range(5):
                        nrow[5 * g + j : 5 * g + j + 1, :] = nout[g : g + 1, 128 * j : 128 * (j + 1)]
                on[...] = nrow[...].astype(BF16)
                to_partner_norm.start()

    arrived(place(z, 1 - c, (0, rows)), p_recv.at[0, 0, 0])
    for h in (1, 2, 3, 4):
        for i in range(len(HOP)):
            for d in range(2):
                if h == 4 and i not in LAST[d]:
                    continue
                arrived(place(z + h * step[d], 1 - c, HOP[i]), p_recv.at[d, h, i])
    for cp in sends:
        cp.wait_send()

    for k in (1, 2, 3):
        chips_sums(k).wait_send()

    @pl.when(c == 1)
    def _():
        for cp in (chips_sums(4), swap(4, 4)):
            cp.wait_send()
        to_partner_norm.wait_recv()

    @pl.when(c == 0)
    def _():
        swap(1, 3).wait_send()
        for cp in (*to_ranks, to_partner_norm):
            cp.wait_send()


def flush(out, fq, fk, fv, on, oq, ok, ov, gq, gk, gv, gn, sem):
    nq, nk = oq.shape[1], ok.shape[1]
    n = out.shape[0] // 4
    pairs = [(fq, gq), (fk, gk), (fv, gv), (on, gn)]
    for k in range(4):
        piece = pl.ds(k * n, n)
        for dst, first, m in ((oq, 0, nq), (ok, nq, nk), (ov, nq + nk, nk)):
            pairs.append((out.at[piece, pl.ds(first, m)], dst.at[piece]))
    copies = [pltpu.make_async_copy(src, dst, sem.at[i]) for i, (src, dst) in enumerate(pairs)]
    for cp in copies:
        cp.start()
    for cp in copies:
        cp.wait()


def per_device(wq, lq, hq, wk, lk, hk, wv, lv, hv, nt, ns):
    rows = wq.shape[0]
    dma = pltpu.SemaphoreType.DMA
    hbm = pl.BlockSpec(memory_space=pltpu.HBM)
    vm = pl.BlockSpec(memory_space=pltpu.VMEM)
    widths = (wq.shape[1], wk.shape[1], wv.shape[1])
    rank = hq.shape[0]
    wide = sum(widths)
    out_shape = (
        pltpu.VMEM((16 * rows, wide), BF16),
        *(pltpu.VMEM((1, m), F32) for m in widths),
        pltpu.VMEM((20, 128), BF16),
    )
    scratch = (
        pltpu.VMEM((rows, wide), BF16),
        pltpu.VMEM((3, rank, rows), BF16),
        pltpu.VMEM((rank, wide), BF16),
        pltpu.VMEM((40,), F32),
        pltpu.VMEM((40,), F32),
        pltpu.VMEM((2, rows, wide), BF16),
        pltpu.VMEM((2, 3, rank, rows), BF16),
        pltpu.VMEM((3, rows, wide), F32),
        pltpu.VMEM((GROUPS + 1, 1, 128), F32),
        pltpu.VMEM((GROUPS + 1, 1, 128), F32),
        pltpu.VMEM((8, GROUPS + 2, 1, 128), F32),
        pltpu.VMEM((8, 2, 1, 128), F32),
        pltpu.VMEM((4, 8, 2, 1, 128), F32),
        pltpu.VMEM((1, wide), F32),
        pltpu.VMEM((4, 640), F32),
        pltpu.VMEM((20, 128), F32),
        dma((11,)),
        pltpu.SemaphoreType.REGULAR,
        pltpu.SemaphoreType.REGULAR((3,)),
        pltpu.SemaphoreType.REGULAR,
        dma, dma,
        dma((4,)), dma((4,)),
        dma, dma,
        dma((3,)), dma((3,)),
        dma, dma,
        dma((2,)), dma((2,)),
        dma((2, 3)), dma((2, 3)),
        dma((2, len(RAW[1]))), dma((2, len(RAW[1]))),
        dma((2, 4, len(HOP))), dma((2, 4, len(HOP))),
        dma((2, 5, len(HOP))), dma((2, 5, len(HOP))),
    )
    made = pl.pallas_call(
        kernel,
        out_shape=out_shape,
        in_specs=[hbm] * 11,
        out_specs=(vm,) * 5,
        scratch_shapes=scratch,
        compiler_params=pltpu.CompilerParams(
            collective_id=0, has_side_effects=True, vmem_limit_bytes=24 * 1024 * 1024
        ),
    )(*(pltpu.with_memory_space_constraint(a, pltpu.HBM) for a in (wq, lq.T, hq, wk, lk.T, hk, wv, lv.T, hv, nt, ns)))
    oq, ok, ov, fq, fk, fv, on = pl.pallas_call(
        flush,
        out_shape=(
            *(jax.ShapeDtypeStruct((16 * rows, m), BF16) for m in widths),
            *(jax.ShapeDtypeStruct((1, m), F32) for m in widths),
            jax.ShapeDtypeStruct((20, 128), BF16),
        ),
        in_specs=[vm] * 5,
        out_specs=(hbm,) * 7,
        scratch_shapes=(dma((16,)),),
        compiler_params=pltpu.CompilerParams(vmem_limit_bytes=1024 * 1024),
    )(*(pltpu.with_memory_space_constraint(a, pltpu.VMEM) for a in made))
    return oq, ok, ov, fq.reshape(-1), fk.reshape(-1), fv.reshape(-1), on.reshape(-1)


def solution(mesh):
    return jax.shard_map(
        per_device,
        mesh=mesh,
        in_specs=(
            P(("shift", "shard"), "tp"),
            P(("shift", "shard"), None),
            P("shift", "tp"),
            P(("shift", "shard"), "tp"),
            P(("shift", "shard"), None),
            P("shift", "tp"),
            P(("shift", "shard"), "tp"),
            P(("shift", "shard"), None),
            P("shift", "tp"),
            P(("shift", "shard", "tp")),
            P(("shift", "shard", "tp")),
        ),
        out_specs=(
            P("shift", "tp"),
            P("shift", "tp"),
            P("shift", "tp"),
            P(("shift", "tp")),
            P(("shift", "tp")),
            P(("shift", "tp")),
            P("shift"),
        ),
        check_vma=False,
    )
```

```python
import functools

import jax
import jax.numpy as jnp
from jax import lax
from jax.experimental import pallas as pl
from jax.experimental.pallas import tpu as pltpu
from jax.sharding import PartitionSpec as P

MESH = pl.DeviceIdType.MESH
F32 = jnp.float32
BF16 = jnp.bfloat16

mix_rate = 1.0

RAW = (((0, 80), (80, 80)),) * 2
HOP = ((0, 80), (80, 80))
LAST = ((0,), (1,))
TILE = 256
GROUPS = 12


def kernel(
    wq, lq, hq, wk, lk, hk, wv, lv, hv, nt, ns,
    out, fq, fk, fv, on,
    own, low, high, snt, sns, raw, pack, rlow, prod, st, stp, sums, gains, nall, inv, nout, nrow,
    load_sem, near, far, ranks, st_send, st_recv, g_send, g_recv, f_send, f_recv, y_send, y_recv, on_send, on_recv,
    low_send, low_recv, ly_send, ly_recv, raw_send, raw_recv, r_send, r_recv, p_send, p_recv,
):
    shard = lax.axis_index("shard")
    y = lax.axis_index("tp")
    z, c = shard // 2, shard % 2
    nz, ny = 8, 4
    rows, wide = own.shape
    d_model = rows * 16
    step = (1 - 2 * c, 2 * c - 1)

    def at(zz, cc):
        return {"shard": lax.rem(zz + 4 * nz, nz) * 2 + cc}

    def rank_of(d):
        return {"tp": lax.rem(y + d, ny)}

    partner = at(z, 1 - c)
    nbr = (at(z + step[0], c), at(z + step[1], c))

    nq, nk = wq.shape[1], wk.shape[1]
    parts = (pl.ds(0, nq), pl.ds(nq, nk), pl.ds(nq + nk, nk))
    pairs = (
        (lq, low.at[0]), (lk, low.at[1]), (lv, low.at[2]),
        (wq, own.at[:, parts[0]]), (wk, own.at[:, parts[1]]), (wv, own.at[:, parts[2]]),
        (hq, high.at[:, parts[0]]), (hk, high.at[:, parts[1]]), (hv, high.at[:, parts[2]]),
        (nt, snt), (ns, sns),
    )
    loads = [pltpu.make_async_copy(src, dst, load_sem.at[i]) for i, (src, dst) in enumerate(pairs)]
    for cp in loads:
        cp.start()

    barrier = pltpu.get_barrier_semaphore()

    def signal(sem, to):
        pl.semaphore_signal(sem, inc=1, device_id=to, device_id_type=MESH)

    for peer in (at(z - 1, 1), at(z + 1, 1)):
        signal(barrier, peer)

    @pl.when(c == 0)
    def _():
        signal(barrier, partner)

    @pl.when(c == 1)
    def _():
        pl.semaphore_wait(barrier, 5)
        signal(near, partner)

    @pl.when(c == 0)
    def _():
        pl.semaphore_wait(near, 1)
        for d in range(1, ny):
            signal(barrier, rank_of(d))

    def pass_on(k):
        signal(far.at[k - 1], nbr[0])

    def heard(k):
        pl.semaphore_wait(far.at[k - 1], 1)

    pass_on(1)

    sends = []

    def send(src, dst, s_sem, r_sem, to):
        cp = pltpu.make_async_remote_copy(
            src_ref=src, dst_ref=dst, send_sem=s_sem, recv_sem=r_sem, device_id=to, device_id_type=MESH
        )
        cp.start()
        sends.append(cp)

    def arrived(dst, sem):
        pltpu.make_async_remote_copy(
            src_ref=dst, dst_ref=dst, send_sem=sem, recv_sem=sem, device_id=partner, device_id_type=MESH
        ).wait_recv()

    def send_raw(d, i):
        piece = pl.ds(*RAW[d][i])
        send(own.at[piece], raw.at[d, piece], raw_send.at[d, i], raw_recv.at[d, i], nbr[d])

    def quarter(rank):
        share = low.shape[1] // ny
        return pl.ds(pl.multiple_of(rank * share, share), share)

    for i in range(3):
        loads[i].wait()
    rest = rows - 128
    pack[:, 384:512] = jnp.zeros((pack.shape[0], 128), BF16)
    for a in range(3):
        share = low[a, quarter(y), :]
        pack[:, 128 * a : 128 * (a + 1)] = share[:, 0:128]
        pack[:, 384 + rest * a : 384 + rest * (a + 1)] = share[:, 128:rows]
    for i in range(3, 6):
        loads[i].wait()
    for d in range(2):
        send(pack, rlow.at[d, quarter(y)], low_send.at[d], low_recv.at[d], nbr[d])
    for d in range(2):
        send_raw(d, 0)
    for i in range(6, 11):
        loads[i].wait()

    def array_of(col):
        return 0 if col < nq else 1 if col < nq + nk else 2

    def product(factor, col):
        return mix_rate * lax.dot_general(
            factor, high[:, col : col + TILE], (((0,), (0,)), ((), ())), preferred_element_type=F32
        )

    for col in range(0, wide, TILE):
        fresh = own[:, col : col + TILE].astype(F32) + product(low[array_of(col)], col)
        prod[2, :, col : col + TILE] = fresh
        total = jnp.sum(jnp.abs(fresh), axis=0, keepdims=True)
        for g in range(TILE // 128):
            j = col // 128 + g
            st[j] = total[:, 128 * g : 128 * (g + 1)]
    st[GROUPS] = jnp.zeros((1, 128), F32)
    st[GROUPS, 0:1, 0:40] = (snt[...] + sns[...]).reshape(1, 40)
    send(st, stp, st_send, st_recv, partner)
    heard(1)
    pass_on(2)
    arrived(stp, st_recv)
    sums[0, 0:GROUPS] = st[0:GROUPS] + stp[0:GROUPS]
    sums[0, GROUPS + c] = st[GROUPS]
    sums[0, GROUPS + 1 - c] = stp[GROUPS]

    def slot(k):
        return k + c * (nz - 2 * k)

    def chips_sums(k):
        return pltpu.make_async_remote_copy(
            src_ref=sums.at[0], dst_ref=sums.at[slot(k)], send_sem=g_send.at[k - 1], recv_sem=g_recv.at[k - 1],
            device_id=at(z + k * step[1], c), device_id_type=MESH,
        )

    for k in (1, 2):
        chips_sums(k).start()
    heard(2)
    pass_on(3)
    chips_sums(3).start()
    heard(3)

    @pl.when(c == 1)
    def _():
        chips_sums(4).start()

    for i in range(1, len(RAW[1])):
        for d in range(2):
            send_raw(d, i)

    @pl.when(c == 0)
    def _():
        pl.semaphore_wait(barrier, ny - 1)
        signal(ranks, partner)

    @pl.when(c == 1)
    def _():
        pl.semaphore_wait(ranks, 1)

    for d in range(2):
        mine = rlow.at[d, quarter(y)]
        arrived(mine, low_recv.at[d])
        for k in range(1, ny):
            send(mine, mine, ly_send.at[d, k - 1], ly_recv.at[d, k - 1], rank_of(k))
    for d in range(2):
        for k in range(1, ny):
            arrived(rlow.at[d, quarter(lax.rem(y - k + ny, ny))], ly_recv.at[d, k - 1])
        for col in range(0, wide, TILE):
            a = array_of(col)
            prod[d, 0:128, col : col + TILE] = product(rlow[d, :, 128 * a : 128 * (a + 1)], col)
            prod[d, 128:rows, col : col + TILE] = product(rlow[d, :, 384 + rest * a : 384 + rest * (a + 1)], col)

    def swap(first, n):
        part = sums.at[pl.ds(first, n)]
        return pltpu.make_async_remote_copy(
            src_ref=part, dst_ref=part, send_sem=f_send, recv_sem=f_recv, device_id=partner, device_id_type=MESH
        )

    for k in (1, 2, 3):
        chips_sums(k).wait_recv()

    @pl.when(c == 0)
    def _():
        swap(1, 3).start()
        swap(4, 4).wait_recv()

    @pl.when(c == 1)
    def _():
        chips_sums(4).wait_recv()
        swap(4, 4).start()
        swap(1, 3).wait_recv()

    total = sums[lax.rem(nz - z, nz), 0:GROUPS]
    for k in range(1, nz):
        total = total + sums[lax.rem(k - z + nz, nz), 0:GROUPS]
    total = total * (1.0 / d_model)
    for j in range(GROUPS):
        factor = total[j]
        inv[:, 128 * j : 128 * (j + 1)] = 1.0 / factor
        if j < 8:
            fq[:, 128 * j : 128 * (j + 1)] = factor
        elif j < 10:
            fk[:, 128 * (j - 8) : 128 * (j - 7)] = factor
        else:
            fv[:, 128 * (j - 10) : 128 * (j - 9)] = factor

    def place(zz, cc, piece):
        first = pl.multiple_of((lax.rem(zz + 4 * nz, nz) * 2 + cc) * rows, 16)
        return out.at[pl.ds(first + piece[0], piece[1])]

    def origin(d, h):
        return z - h * step[d]

    def to_partner(d, h, i):
        dst = place(origin(d, h), c, HOP[i])
        send(dst, dst, p_send.at[d, h, i], p_recv.at[d, h, i], partner)

    def onward(d, h, i):
        dst = place(origin(d, h), c, HOP[i])
        send(dst, dst, r_send.at[d, h, i], r_recv.at[d, h, i], nbr[d])

    for i, (h0, hn) in enumerate(HOP):
        for d in range(2):
            for j, (r0, n) in enumerate(RAW[d]):
                if not h0 <= r0 < h0 + hn:
                    continue
                arrived(raw.at[d, pl.ds(r0, n)], raw_recv.at[d, j])
                dst = place(origin(d, 1), c, (r0, n))
                for col in range(0, wide, TILE):
                    fresh = raw[d, r0 : r0 + n, col : col + TILE].astype(F32) + prod[d, r0 : r0 + n, col : col + TILE]
                    dst[:, col : col + TILE] = (fresh * inv[:, col : col + TILE]).astype(BF16)
            onward(d, 1, i)
            to_partner(d, 1, i)
    dst = place(z, c, (0, rows))
    for col in range(0, wide, TILE):
        dst[:, col : col + TILE] = (prod[2, :, col : col + TILE] * inv[:, col : col + TILE]).astype(BF16)
    send(dst, dst, p_send.at[0, 0, 0], p_recv.at[0, 0, 0], partner)

    to_ranks = [
        pltpu.make_async_remote_copy(
            src_ref=gains, dst_ref=nall.at[y], send_sem=y_send.at[d - 1], recv_sem=y_recv.at[d - 1],
            device_id=rank_of(d), device_id_type=MESH,
        )
        for d in range(1, ny)
    ]
    to_partner_norm = pltpu.make_async_remote_copy(
        src_ref=on, dst_ref=on, send_sem=on_send, recv_sem=on_recv, device_id=partner, device_id_type=MESH
    )

    @pl.when(c == 0)
    def _():
        for k in range(nz):
            gains[k] = sums[lax.rem(k - z + nz, nz), GROUPS : GROUPS + 2]
        nall[y] = gains[...]
        for cp in to_ranks:
            cp.start()

    for h in (2, 3, 4):
        for i in range(len(HOP)):
            for d in range(2):
                if h == 4 and i not in LAST[d]:
                    continue
                arrived(place(origin(d, h), c, HOP[i]), r_recv.at[d, h - 1, i])
                if h == 2 or (h == 3 and i in LAST[d]):
                    onward(d, h, i)
                to_partner(d, h, i)
        if h == 2:

            @pl.when(c == 0)
            def _():
                for d in range(1, ny):
                    arrived(nall.at[lax.rem(y - d + ny, ny)], y_recv.at[d - 1])
                for b in range(4):
                    for yy in range(ny):
                        k = 4 * b + yy
                        for g in range(4):
                            s = 4 * g + b
                            nout[g : g + 1, 40 * k : 40 * k + 40] = nall[yy, s // 2, s % 2, :, 0:40]
                for g in range(4):
                    for j in range(5):
                        nrow[5 * g + j : 5 * g + j + 1, :] = nout[g : g + 1, 128 * j : 128 * (j + 1)]
                on[...] = nrow[...].astype(BF16)
                to_partner_norm.start()

    arrived(place(z, 1 - c, (0, rows)), p_recv.at[0, 0, 0])
    for h in (1, 2, 3, 4):
        for i in range(len(HOP)):
            for d in range(2):
                if h == 4 and i not in LAST[d]:
                    continue
                arrived(place(z + h * step[d], 1 - c, HOP[i]), p_recv.at[d, h, i])
    for cp in sends:
        cp.wait_send()

    for k in (1, 2, 3):
        chips_sums(k).wait_send()

    @pl.when(c == 1)
    def _():
        for cp in (chips_sums(4), swap(4, 4)):
            cp.wait_send()
        to_partner_norm.wait_recv()

    @pl.when(c == 0)
    def _():
        swap(1, 3).wait_send()
        for cp in (*to_ranks, to_partner_norm):
            cp.wait_send()


def flush(out, fq, fk, fv, on, oq, ok, ov, gq, gk, gv, gn, sem):
    nq, nk = oq.shape[1], ok.shape[1]
    n = out.shape[0] // 4
    pairs = [(fq, gq), (fk, gk), (fv, gv), (on, gn)]
    for k in range(4):
        piece = pl.ds(k * n, n)
        for dst, first, m in ((oq, 0, nq), (ok, nq, nk), (ov, nq + nk, nk)):
            pairs.append((out.at[piece, pl.ds(first, m)], dst.at[piece]))
    copies = [pltpu.make_async_copy(src, dst, sem.at[i]) for i, (src, dst) in enumerate(pairs)]
    for cp in copies:
        cp.start()
    for cp in copies:
        cp.wait()


def per_device(wq, lq, hq, wk, lk, hk, wv, lv, hv, nt, ns):
    rows = wq.shape[0]
    dma = pltpu.SemaphoreType.DMA
    hbm = pl.BlockSpec(memory_space=pltpu.HBM)
    vm = pl.BlockSpec(memory_space=pltpu.VMEM)
    widths = (wq.shape[1], wk.shape[1], wv.shape[1])
    rank = hq.shape[0]
    wide = sum(widths)
    out_shape = (
        pltpu.VMEM((16 * rows, wide), BF16),
        *(pltpu.VMEM((1, m), F32) for m in widths),
        pltpu.VMEM((20, 128), BF16),
    )
    scratch = (
        pltpu.VMEM((rows, wide), BF16),
        pltpu.VMEM((3, rank, rows), BF16),
        pltpu.VMEM((rank, wide), BF16),
        pltpu.VMEM((40,), F32),
        pltpu.VMEM((40,), F32),
        pltpu.VMEM((2, rows, wide), BF16),
        pltpu.VMEM((rank // 4, 512), BF16),
        pltpu.VMEM((2, rank, 512), BF16),
        pltpu.VMEM((3, rows, wide), F32),
        pltpu.VMEM((GROUPS + 1, 1, 128), F32),
        pltpu.VMEM((GROUPS + 1, 1, 128), F32),
        pltpu.VMEM((8, GROUPS + 2, 1, 128), F32),
        pltpu.VMEM((8, 2, 1, 128), F32),
        pltpu.VMEM((4, 8, 2, 1, 128), F32),
        pltpu.VMEM((1, wide), F32),
        pltpu.VMEM((4, 640), F32),
        pltpu.VMEM((20, 128), F32),
        dma((11,)),
        pltpu.SemaphoreType.REGULAR,
        pltpu.SemaphoreType.REGULAR((3,)),
        pltpu.SemaphoreType.REGULAR,
        dma, dma,
        dma((4,)), dma((4,)),
        dma, dma,
        dma((3,)), dma((3,)),
        dma, dma,
        dma((2,)), dma((2,)),
        dma((2, 3)), dma((2, 3)),
        dma((2, len(RAW[1]))), dma((2, len(RAW[1]))),
        dma((2, 4, len(HOP))), dma((2, 4, len(HOP))),
        dma((2, 5, len(HOP))), dma((2, 5, len(HOP))),
    )
    made = pl.pallas_call(
        kernel,
        out_shape=out_shape,
        in_specs=[hbm] * 11,
        out_specs=(vm,) * 5,
        scratch_shapes=scratch,
        compiler_params=pltpu.CompilerParams(
            collective_id=0, has_side_effects=True, vmem_limit_bytes=24 * 1024 * 1024
        ),
    )(*(pltpu.with_memory_space_constraint(a, pltpu.HBM) for a in (wq, lq.T, hq, wk, lk.T, hk, wv, lv.T, hv, nt, ns)))
    oq, ok, ov, fq, fk, fv, on = pl.pallas_call(
        flush,
        out_shape=(
            *(jax.ShapeDtypeStruct((16 * rows, m), BF16) for m in widths),
            *(jax.ShapeDtypeStruct((1, m), F32) for m in widths),
            jax.ShapeDtypeStruct((20, 128), BF16),
        ),
        in_specs=[vm] * 5,
        out_specs=(hbm,) * 7,
        scratch_shapes=(dma((16,)),),
        compiler_params=pltpu.CompilerParams(vmem_limit_bytes=1024 * 1024),
    )(*(pltpu.with_memory_space_constraint(a, pltpu.VMEM) for a in made))
    return oq, ok, ov, fq.reshape(-1), fk.reshape(-1), fv.reshape(-1), on.reshape(-1)


def solution(mesh):
    return jax.shard_map(
        per_device,
        mesh=mesh,
        in_specs=(
            P(("shift", "shard"), "tp"),
            P(("shift", "shard"), None),
            P("shift", "tp"),
            P(("shift", "shard"), "tp"),
            P(("shift", "shard"), None),
            P("shift", "tp"),
            P(("shift", "shard"), "tp"),
            P(("shift", "shard"), None),
            P("shift", "tp"),
            P(("shift", "shard", "tp")),
            P(("shift", "shard", "tp")),
        ),
        out_specs=(
            P("shift", "tp"),
            P("shift", "tp"),
            P("shift", "tp"),
            P(("shift", "tp")),
            P(("shift", "tp")),
            P(("shift", "tp")),
            P("shift"),
        ),
        check_vma=False,
    )
```

```python
import functools

import jax
import jax.numpy as jnp
from jax import lax
from jax.experimental import pallas as pl
from jax.experimental.pallas import tpu as pltpu
from jax.sharding import PartitionSpec as P

MESH = pl.DeviceIdType.MESH
F32 = jnp.float32
BF16 = jnp.bfloat16

mix_rate = 1.0

RAW = (((0, 80), (80, 80)),) * 2
HOP = ((0, 80), (80, 80))
LAST = ((0,), (1,))
TILE = 256
GROUPS = 12


def kernel(
    wq, lq, hq, wk, lk, hk, wv, lv, hv, nt, ns,
    out, fq, fk, fv, on,
    own, low, high, snt, sns, raw, rlow, prod, st, stp, sums, gains, nall, inv, nout, nrow,
    load_sem, near, far, ranks, st_send, st_recv, g_send, g_recv, f_send, f_recv, y_send, y_recv, on_send, on_recv,
    low_send, low_recv, ly_send, ly_recv, raw_send, raw_recv, r_send, r_recv, p_send, p_recv,
):
    shard = lax.axis_index("shard")
    y = lax.axis_index("tp")
    z, c = shard // 2, shard % 2
    nz, ny = 8, 4
    rows, wide = own.shape
    d_model = rows * 16
    step = (1 - 2 * c, 2 * c - 1)

    def at(zz, cc):
        return {"shard": lax.rem(zz + 4 * nz, nz) * 2 + cc}

    def rank_of(d):
        return {"tp": lax.rem(y + d, ny)}

    partner = at(z, 1 - c)
    nbr = (at(z + step[0], c), at(z + step[1], c))

    nq, nk = wq.shape[1], wk.shape[1]
    parts = (pl.ds(0, nq), pl.ds(nq, nk), pl.ds(nq + nk, nk))
    pairs = (
        (lq, low.at[0]), (lk, low.at[1]), (lv, low.at[2]),
        (wq, own.at[:, parts[0]]), (wk, own.at[:, parts[1]]), (wv, own.at[:, parts[2]]),
        (hq, high.at[:, parts[0]]), (hk, high.at[:, parts[1]]), (hv, high.at[:, parts[2]]),
        (nt, snt), (ns, sns),
    )
    loads = [pltpu.make_async_copy(src, dst, load_sem.at[i]) for i, (src, dst) in enumerate(pairs)]
    for cp in loads:
        cp.start()

    barrier = pltpu.get_barrier_semaphore()

    def signal(sem, to):
        pl.semaphore_signal(sem, inc=1, device_id=to, device_id_type=MESH)

    for peer in (at(z - 1, 1), at(z + 1, 1)):
        signal(barrier, peer)

    @pl.when(c == 0)
    def _():
        signal(barrier, partner)

    @pl.when(c == 1)
    def _():
        pl.semaphore_wait(barrier, 5)
        signal(near, partner)

    @pl.when(c == 0)
    def _():
        pl.semaphore_wait(near, 1)
        for d in range(1, ny):
            signal(barrier, rank_of(d))

    def pass_on(k):
        signal(far.at[k - 1], nbr[0])

    def heard(k):
        pl.semaphore_wait(far.at[k - 1], 1)

    pass_on(1)

    sends = []

    def send(src, dst, s_sem, r_sem, to):
        cp = pltpu.make_async_remote_copy(
            src_ref=src, dst_ref=dst, send_sem=s_sem, recv_sem=r_sem, device_id=to, device_id_type=MESH
        )
        cp.start()
        sends.append(cp)

    def arrived(dst, sem):
        pltpu.make_async_remote_copy(
            src_ref=dst, dst_ref=dst, send_sem=sem, recv_sem=sem, device_id=partner, device_id_type=MESH
        ).wait_recv()

    def send_raw(d, i):
        piece = pl.ds(*RAW[d][i])
        send(own.at[piece], raw.at[d, piece], raw_send.at[d, i], raw_recv.at[d, i], nbr[d])

    def quarter(rank):
        share = low.shape[1] // ny
        return pl.ds(pl.multiple_of(rank * share, share), share)

    for i in range(3):
        loads[i].wait()
    for d in range(2):
        send(low.at[:, quarter(y)], rlow.at[d, :, quarter(y)], low_send.at[d], low_recv.at[d], nbr[d])
    for i in range(3, 6):
        loads[i].wait()
    for d in range(2):
        send_raw(d, 0)
    for i in range(6, 11):
        loads[i].wait()

    def array_of(col):
        return 0 if col < nq else 1 if col < nq + nk else 2

    def product(l_ref, col):
        return mix_rate * lax.dot_general(
            l_ref[array_of(col)], high[:, col : col + TILE], (((0,), (0,)), ((), ())), preferred_element_type=F32
        )

    for col in range(0, wide, TILE):
        fresh = own[:, col : col + TILE].astype(F32) + product(low, col)
        prod[2, :, col : col + TILE] = fresh
        total = jnp.sum(jnp.abs(fresh), axis=0, keepdims=True)
        for g in range(TILE // 128):
            j = col // 128 + g
            st[j] = total[:, 128 * g : 128 * (g + 1)]
    st[GROUPS] = jnp.zeros((1, 128), F32)
    st[GROUPS, 0:1, 0:40] = (snt[...] + sns[...]).reshape(1, 40)
    send(st, stp, st_send, st_recv, partner)
    heard(1)
    pass_on(2)
    arrived(stp, st_recv)
    sums[0, 0:GROUPS] = st[0:GROUPS] + stp[0:GROUPS]
    sums[0, GROUPS + c] = st[GROUPS]
    sums[0, GROUPS + 1 - c] = stp[GROUPS]

    def slot(k):
        return k + c * (nz - 2 * k)

    def chips_sums(k):
        return pltpu.make_async_remote_copy(
            src_ref=sums.at[0], dst_ref=sums.at[slot(k)], send_sem=g_send.at[k - 1], recv_sem=g_recv.at[k - 1],
            device_id=at(z + k * step[1], c), device_id_type=MESH,
        )

    for k in (1, 2):
        chips_sums(k).start()
    heard(2)
    pass_on(3)
    chips_sums(3).start()
    heard(3)

    @pl.when(c == 1)
    def _():
        chips_sums(4).start()

    for i in range(1, len(RAW[1])):
        for d in range(2):
            send_raw(d, i)

    @pl.when(c == 0)
    def _():
        pl.semaphore_wait(barrier, ny - 1)
        signal(ranks, partner)

    @pl.when(c == 1)
    def _():
        pl.semaphore_wait(ranks, 1)

    for d in range(2):
        mine = rlow.at[d, :, quarter(y)]
        arrived(mine, low_recv.at[d])
        for k in range(1, ny):
            send(mine, mine, ly_send.at[d, k - 1], ly_recv.at[d, k - 1], rank_of(k))
    for d in range(2):
        for k in range(1, ny):
            arrived(rlow.at[d, :, quarter(lax.rem(y - k + ny, ny))], ly_recv.at[d, k - 1])
        for col in range(0, wide, TILE):
            prod[d, :, col : col + TILE] = product(rlow.at[d], col)

    def swap(first, n):
        part = sums.at[pl.ds(first, n)]
        return pltpu.make_async_remote_copy(
            src_ref=part, dst_ref=part, send_sem=f_send, recv_sem=f_recv, device_id=partner, device_id_type=MESH
        )

    for k in (1, 2, 3):
        chips_sums(k).wait_recv()

    @pl.when(c == 0)
    def _():
        swap(1, 3).start()
        swap(4, 4).wait_recv()

    @pl.when(c == 1)
    def _():
        chips_sums(4).wait_recv()
        swap(4, 4).start()
        swap(1, 3).wait_recv()

    total = sums[lax.rem(nz - z, nz), 0:GROUPS]
    for k in range(1, nz):
        total = total + sums[lax.rem(k - z + nz, nz), 0:GROUPS]
    total = total * (1.0 / d_model)
    for j in range(GROUPS):
        factor = total[j]
        inv[:, 128 * j : 128 * (j + 1)] = 1.0 / factor
        if j < 8:
            fq[:, 128 * j : 128 * (j + 1)] = factor
        elif j < 10:
            fk[:, 128 * (j - 8) : 128 * (j - 7)] = factor
        else:
            fv[:, 128 * (j - 10) : 128 * (j - 9)] = factor

    def place(zz, cc, piece):
        first = pl.multiple_of((lax.rem(zz + 4 * nz, nz) * 2 + cc) * rows, 16)
        return out.at[pl.ds(first + piece[0], piece[1])]

    def origin(d, h):
        return z - h * step[d]

    def to_partner(d, h, i):
        dst = place(origin(d, h), c, HOP[i])
        send(dst, dst, p_send.at[d, h, i], p_recv.at[d, h, i], partner)

    def onward(d, h, i):
        dst = place(origin(d, h), c, HOP[i])
        send(dst, dst, r_send.at[d, h, i], r_recv.at[d, h, i], nbr[d])

    for i, (h0, hn) in enumerate(HOP):
        for d in range(2):
            for j, (r0, n) in enumerate(RAW[d]):
                if not h0 <= r0 < h0 + hn:
                    continue
                arrived(raw.at[d, pl.ds(r0, n)], raw_recv.at[d, j])
                dst = place(origin(d, 1), c, (r0, n))
                for col in range(0, wide, TILE):
                    fresh = raw[d, r0 : r0 + n, col : col + TILE].astype(F32) + prod[d, r0 : r0 + n, col : col + TILE]
                    dst[:, col : col + TILE] = (fresh * inv[:, col : col + TILE]).astype(BF16)
            to_partner(d, 1, i)
            onward(d, 1, i)
    dst = place(z, c, (0, rows))
    for col in range(0, wide, TILE):
        dst[:, col : col + TILE] = (prod[2, :, col : col + TILE] * inv[:, col : col + TILE]).astype(BF16)
    send(dst, dst, p_send.at[0, 0, 0], p_recv.at[0, 0, 0], partner)

    to_ranks = [
        pltpu.make_async_remote_copy(
            src_ref=gains, dst_ref=nall.at[y], send_sem=y_send.at[d - 1], recv_sem=y_recv.at[d - 1],
            device_id=rank_of(d), device_id_type=MESH,
        )
        for d in range(1, ny)
    ]
    to_partner_norm = pltpu.make_async_remote_copy(
        src_ref=on, dst_ref=on, send_sem=on_send, recv_sem=on_recv, device_id=partner, device_id_type=MESH
    )

    @pl.when(c == 0)
    def _():
        for k in range(nz):
            gains[k] = sums[lax.rem(k - z + nz, nz), GROUPS : GROUPS + 2]
        nall[y] = gains[...]
        for cp in to_ranks:
            cp.start()

    for h in (2, 3, 4):
        for i in range(len(HOP)):
            for d in (1, 0):
                if h == 4 and i not in LAST[d]:
                    continue
                arrived(place(origin(d, h), c, HOP[i]), r_recv.at[d, h - 1, i])
                if h == 2 or (h == 3 and i in LAST[d]):
                    onward(d, h, i)
                to_partner(d, h, i)
        if h == 2:

            @pl.when(c == 0)
            def _():
                for d in range(1, ny):
                    arrived(nall.at[lax.rem(y - d + ny, ny)], y_recv.at[d - 1])
                for b in range(4):
                    for yy in range(ny):
                        k = 4 * b + yy
                        for g in range(4):
                            s = 4 * g + b
                            nout[g : g + 1, 40 * k : 40 * k + 40] = nall[yy, s // 2, s % 2, :, 0:40]
                for g in range(4):
                    for j in range(5):
                        nrow[5 * g + j : 5 * g + j + 1, :] = nout[g : g + 1, 128 * j : 128 * (j + 1)]
                on[...] = nrow[...].astype(BF16)
                to_partner_norm.start()

    arrived(place(z, 1 - c, (0, rows)), p_recv.at[0, 0, 0])
    for h in (1, 2, 3, 4):
        for i in range(len(HOP)):
            for d in range(2):
                if h == 4 and i not in LAST[d]:
                    continue
                arrived(place(z + h * step[d], 1 - c, HOP[i]), p_recv.at[d, h, i])
    for cp in sends:
        cp.wait_send()

    for k in (1, 2, 3):
        chips_sums(k).wait_send()

    @pl.when(c == 1)
    def _():
        for cp in (chips_sums(4), swap(4, 4)):
            cp.wait_send()
        to_partner_norm.wait_recv()

    @pl.when(c == 0)
    def _():
        swap(1, 3).wait_send()
        for cp in (*to_ranks, to_partner_norm):
            cp.wait_send()


def flush(out, fq, fk, fv, on, oq, ok, ov, gq, gk, gv, gn, sem):
    nq, nk = oq.shape[1], ok.shape[1]
    n = out.shape[0] // 4
    pairs = [(fq, gq), (fk, gk), (fv, gv), (on, gn)]
    for k in range(4):
        piece = pl.ds(k * n, n)
        for dst, first, m in ((oq, 0, nq), (ok, nq, nk), (ov, nq + nk, nk)):
            pairs.append((out.at[piece, pl.ds(first, m)], dst.at[piece]))
    copies = [pltpu.make_async_copy(src, dst, sem.at[i]) for i, (src, dst) in enumerate(pairs)]
    for cp in copies:
        cp.start()
    for cp in copies:
        cp.wait()


def per_device(wq, lq, hq, wk, lk, hk, wv, lv, hv, nt, ns):
    rows = wq.shape[0]
    dma = pltpu.SemaphoreType.DMA
    hbm = pl.BlockSpec(memory_space=pltpu.HBM)
    vm = pl.BlockSpec(memory_space=pltpu.VMEM)
    widths = (wq.shape[1], wk.shape[1], wv.shape[1])
    rank = hq.shape[0]
    wide = sum(widths)
    out_shape = (
        pltpu.VMEM((16 * rows, wide), BF16),
        *(pltpu.VMEM((1, m), F32) for m in widths),
        pltpu.VMEM((20, 128), BF16),
    )
    scratch = (
        pltpu.VMEM((rows, wide), BF16),
        pltpu.VMEM((3, rank, rows), BF16),
        pltpu.VMEM((rank, wide), BF16),
        pltpu.VMEM((40,), F32),
        pltpu.VMEM((40,), F32),
        pltpu.VMEM((2, rows, wide), BF16),
        pltpu.VMEM((2, 3, rank, rows), BF16),
        pltpu.VMEM((3, rows, wide), F32),
        pltpu.VMEM((GROUPS + 1, 1, 128), F32),
        pltpu.VMEM((GROUPS + 1, 1, 128), F32),
        pltpu.VMEM((8, GROUPS + 2, 1, 128), F32),
        pltpu.VMEM((8, 2, 1, 128), F32),
        pltpu.VMEM((4, 8, 2, 1, 128), F32),
        pltpu.VMEM((1, wide), F32),
        pltpu.VMEM((4, 640), F32),
        pltpu.VMEM((20, 128), F32),
        dma((11,)),
        pltpu.SemaphoreType.REGULAR,
        pltpu.SemaphoreType.REGULAR((3,)),
        pltpu.SemaphoreType.REGULAR,
        dma, dma,
        dma((4,)), dma((4,)),
        dma, dma,
        dma((3,)), dma((3,)),
        dma, dma,
        dma((2,)), dma((2,)),
        dma((2, 3)), dma((2, 3)),
        dma((2, len(RAW[1]))), dma((2, len(RAW[1]))),
        dma((2, 4, len(HOP))), dma((2, 4, len(HOP))),
        dma((2, 5, len(HOP))), dma((2, 5, len(HOP))),
    )
    made = pl.pallas_call(
        kernel,
        out_shape=out_shape,
        in_specs=[hbm] * 11,
        out_specs=(vm,) * 5,
        scratch_shapes=scratch,
        compiler_params=pltpu.CompilerParams(
            collective_id=0, has_side_effects=True, vmem_limit_bytes=24 * 1024 * 1024
        ),
    )(*(pltpu.with_memory_space_constraint(a, pltpu.HBM) for a in (wq, lq.T, hq, wk, lk.T, hk, wv, lv.T, hv, nt, ns)))
    oq, ok, ov, fq, fk, fv, on = pl.pallas_call(
        flush,
        out_shape=(
            *(jax.ShapeDtypeStruct((16 * rows, m), BF16) for m in widths),
            *(jax.ShapeDtypeStruct((1, m), F32) for m in widths),
            jax.ShapeDtypeStruct((20, 128), BF16),
        ),
        in_specs=[vm] * 5,
        out_specs=(hbm,) * 7,
        scratch_shapes=(dma((16,)),),
        compiler_params=pltpu.CompilerParams(vmem_limit_bytes=1024 * 1024),
    )(*(pltpu.with_memory_space_constraint(a, pltpu.VMEM) for a in made))
    return oq, ok, ov, fq.reshape(-1), fk.reshape(-1), fv.reshape(-1), on.reshape(-1)


def solution(mesh):
    return jax.shard_map(
        per_device,
        mesh=mesh,
        in_specs=(
            P(("shift", "shard"), "tp"),
            P(("shift", "shard"), None),
            P("shift", "tp"),
            P(("shift", "shard"), "tp"),
            P(("shift", "shard"), None),
            P("shift", "tp"),
            P(("shift", "shard"), "tp"),
            P(("shift", "shard"), None),
            P("shift", "tp"),
            P(("shift", "shard", "tp")),
            P(("shift", "shard", "tp")),
        ),
        out_specs=(
            P("shift", "tp"),
            P("shift", "tp"),
            P("shift", "tp"),
            P(("shift", "tp")),
            P(("shift", "tp")),
            P(("shift", "tp")),
            P("shift"),
        ),
        check_vma=False,
    )
```
